256 devices in a mesh: dp: 16 (over y, x_lo, core), seq: 16 (over x_hi, z).
Axes of the slice: x: 4 (x_hi: 2, x_lo: 2; x = x_hi * 2 + x_lo), y: 4, z: 8, core: 2. Of those that a mesh axis runs over, the one named last changes fastest.
Arguments:
- queries: bfloat16 [65536, 1664], P(('dp', 'seq')), parts along dimension 0, may hold values from -6 to 6
- key_rows: bfloat16 [65536, 1664], P(('dp', 'seq')), parts along dimension 0, may hold values from -6 to 6
- value_rows: bfloat16 [65536, 1664], P(('dp', 'seq')), parts along dimension 0, may hold values from -6 to 6
Outputs:
- merged_tokens: bfloat16 [16384, 6656], P('dp', 'seq'), parts along dimension 0
The draws below stay inside these ranges and needn't reach their ends.
There are 16 independent parts, one for each index of `dp`. The reference program is written for one: setup_inputs(seed, part) draws one part's arguments, and reference() takes and returns one part's arrays. A program takes and returns all parts, laid end to end along the dimension named above; each array names one. Nothing has to cross between parts.
All inputs are finite; a program needn't handle non-finite values.
Results may differ from the reference program's by a relative error of at most 0.005.
Values may be sent and summed in bfloat16 or wider, within the bound.
No kernel may reach another device: no remote copies, remote signals or barrier semaphores. Data moves between devices by JAX's collectives and lax.ppermute only.
A program may use at most 128 MiB of HBM per device.

```python
import math
import jax
import jax.numpy as jnp
from jax import lax

HEADS = 13
HEAD_DIM = 128
GRID_W = 64
TOKENS = 4096
CH = 1664


def draw_pair(key):
    width = HEADS * HEAD_DIM
    query_key = jax.random.fold_in(key, 11)
    other_key = jax.random.fold_in(key, 12)
    queries = 1.6 * jax.random.truncated_normal(query_key, -3.75, 3.75, (TOKENS, width), jnp.float32)
    key_rows = 1.6 * jax.random.truncated_normal(other_key, -3.75, 3.75, (TOKENS, width), jnp.float32)
    return (queries, key_rows)


def draw_queries(key, part):
    return draw_pair(key)[0].astype(jnp.bfloat16)


def draw_key_rows(key, part):
    return draw_pair(key)[1].astype(jnp.bfloat16)


def block_levels(stream_key, shape, split, least, top_value):
    loudness, own = 1.0, jax.random.fold_in(stream_key, 6)
    for axis_at, blocks in split:
        heights = jnp.exp(jax.random.uniform(jax.random.fold_in(own, axis_at), (blocks,), jnp.float32, least / len(split), top_value / len(split)))
        loudness = loudness * jnp.repeat(heights, shape[axis_at] // blocks).reshape([-1 if axis == axis_at else 1 for axis in range(len(shape))])
    return loudness


def centred(own_key, extent, spread, limit, pieces=(), dtype=jnp.bfloat16):
    gain = block_levels(own_key, extent, pieces, -0.22, 0.18) if pieces else 1.0
    drawn = jax.random.normal(own_key, extent, jnp.float32) * spread * gain
    return jnp.minimum(jnp.maximum(drawn, -limit), limit).astype(dtype)


def setup_inputs(seed: int = 0, part: int = 0) -> dict:
    keys = jax.random.split(jax.random.key(seed), 4)
    own_keys = jax.random.split(jax.random.fold_in(keys[3], part), 4)
    queries = draw_queries(jax.random.fold_in(jax.random.fold_in(keys[3], part), 71), part)
    key_rows = draw_key_rows(jax.random.fold_in(jax.random.fold_in(keys[3], part), 71), part)
    value_rows = centred(own_keys[2], (TOKENS, CH), 1.0, 6.0, ((0, 16),))
    return {"queries": queries, "key_rows": key_rows, "value_rows": value_rows}


def one_head(query_head, key_head, value_head):
    total_rows = query_head.shape[0]
    block_rows = math.gcd(total_rows, 512)
    score_scale = 1.0 / math.sqrt(HEAD_DIM)
    blocks = query_head.reshape(total_rows // block_rows, block_rows, HEAD_DIM)

    def attend(query_block):
        scores = jnp.dot(query_block, key_head.T, preferred_element_type=jnp.float32) * score_scale
        row_max = lax.optimization_barrier(jnp.max(scores, axis=-1, keepdims=True))
        weights = jnp.exp(scores - row_max)
        totals = lax.optimization_barrier(jnp.sum(weights, axis=-1, keepdims=True))
        weighted = jnp.dot(weights.astype(jnp.bfloat16), value_head, preferred_element_type=jnp.float32)
        return (weighted / totals).astype(jnp.bfloat16)
    return lax.map(attend, blocks).reshape(total_rows, HEAD_DIM)

def reference(queries, key_rows, value_rows):
    tokens = queries.shape[0]
    query_heads = queries.reshape(tokens, HEADS, HEAD_DIM).transpose(1, 0, 2)
    key_heads = key_rows.reshape(tokens, HEADS, HEAD_DIM).transpose(1, 0, 2)
    value_heads = value_rows.reshape(tokens, HEADS, HEAD_DIM).transpose(1, 0, 2)
    attended = lax.map(lambda triple: one_head(triple[0], triple[1], triple[2]), (query_heads, key_heads, value_heads))
    attended = attended.transpose(1, 0, 2).reshape(tokens, HEADS * HEAD_DIM)
    grid_rows = tokens // GRID_W
    shuffled = attended.reshape(grid_rows // 2, 2, GRID_W // 2, 2, HEADS * HEAD_DIM).transpose(0, 2, 1, 3, 4)
    return shuffled.reshape(grid_rows // 2 * (GRID_W // 2), 4 * HEADS * HEAD_DIM)
```

```python
import math

import jax
import jax.numpy as jnp
import numpy as np
from jax import lax
from jax.experimental import pallas as pl
from jax.experimental.pallas import tpu as pltpu
from jax.sharding import PartitionSpec as P


HEAD_DIM = 128
HEADS = 13
SEQ = 16
TOK = 256
LOC = 64
OUT_COLS = 416
FAR = 1 << 20
LOG2_SCALE = math.log2(math.e) / math.sqrt(HEAD_DIM)


IDLE = (((), (0,), (1,), (3,)), ((), (3,), (2,), (0,)))
CHUNK_HEADS = ((0, 1, 2, 3), (4, 5, 6), (7, 8, 9), (10, 11, 12))

ROTATIONS = ((0, 0), (0, 4), (1, 4), (0, 3), (0, 5), (1, 3), (1, 5), (0, 2), (0, 6), (1, 2), (1, 6), (0, 1), (0, 7),
             (1, 1), (1, 7), (1, 0))
XORS = (3, 1, 2, 0)


def place_heads():
    head_of = np.full((2, SEQ), -1, np.int32)
    for core in range(2):
        for chunk in range(4):
            places = [p for p in range(4) if p not in IDLE[core][chunk]]
            for place, head in zip(places, CHUNK_HEADS[chunk]):
                head_of[core, place * 4 + chunk] = head
    return head_of


HEAD_OF = place_heads()


def turn(seq, rotation, sign=1):
    dx, dz = rotation
    return ((seq // 8) ^ dx) * 8 + (seq % 8 + sign * dz) % 8


def tables():
    send = np.zeros((2, SEQ, 16), np.int32)
    source = np.zeros((2, SEQ, 16), np.int32)
    shift = np.full((2, SEQ, 5), FAR, np.int32)
    for core in range(2):
        for seq in range(SEQ):
            for r, rotation in enumerate(ROTATIONS):
                send[core, seq, r] = max(HEAD_OF[core, turn(seq, rotation)], 0)
                source[core, seq, r] = turn(seq, rotation, -1)
            chunk, place = seq % 4, seq // 4
            for j, flip in enumerate(XORS):
                head = HEAD_OF[core, (place ^ flip) * 4 + chunk]
                if head >= 0:
                    shift[core, seq, j] = head * HEAD_DIM - chunk * OUT_COLS
            if chunk > 0:
                shift[core, seq, 4] = CHUNK_HEADS[chunk - 1][-1] * HEAD_DIM - chunk * OUT_COLS
    return send, source, shift


SEND, SOURCE, SHIFT = tables()


def last_index():
    table = np.zeros((2, SEQ), np.int32)
    for core in range(2):
        for seq in range(SEQ):
            chunk, place = seq % 4, seq // 4
            for j, flip in enumerate(XORS):
                if HEAD_OF[core, (place ^ flip) * 4 + chunk] == CHUNK_HEADS[chunk][-1]:
                    table[core, seq] = j
    return table


LAST = last_index()


def pairs(step, active):
    out = []
    for dp in range(16):
        for seq in range(SEQ):
            target = step(seq)
            if target is not None and active(dp % 2, seq, target):
                out.append((dp * SEQ + seq, dp * SEQ + target))
    return out


def pack_kernel(send_ref, q_ref, k_ref, v_ref, *refs):
    outs, q_sorted = refs[:16], refs[16]
    row = lax.broadcasted_iota(jnp.int32, (TOK, TOK), 0)
    col = lax.broadcasted_iota(jnp.int32, (TOK, TOK), 1)
    grid_row, grid_col = col // 64, col % 64
    wanted = ((grid_row % 2) * 2 + grid_col % 2) * LOC + (grid_row // 2) * 32 + grid_col // 2
    order = jnp.where(row == wanted, 1.0, 0.0).astype(jnp.bfloat16)
    q_sorted[...] = jnp.dot(order, q_ref[...], preferred_element_type=jnp.float32).astype(jnp.bfloat16)
    for r in range(16):
        at = pl.ds(pl.multiple_of(send_ref[r] * HEAD_DIM, HEAD_DIM), HEAD_DIM)
        outs[r][0:TOK, :] = q_sorted[:, at]
        outs[r][TOK:2 * TOK, :] = k_ref[:, at]
        outs[r][2 * TOK:, :] = v_ref[:, at]


def pack(send, queries, key_rows, value_rows):
    shape = jax.ShapeDtypeStruct((3 * TOK, HEAD_DIM), jnp.bfloat16)
    full = pl.BlockSpec(memory_space=pltpu.VMEM)
    return pl.pallas_call(
        pack_kernel,
        in_specs=[pl.BlockSpec(memory_space=pltpu.SMEM), full, full, full],
        out_specs=[full] * 16,
        out_shape=[shape] * 16,
        scratch_shapes=[pltpu.VMEM((TOK, HEADS * HEAD_DIM), jnp.bfloat16)],
        compiler_params=pltpu.CompilerParams(vmem_limit_bytes=24 * 2**20),
        name="pack",
    )(send, queries, key_rows, value_rows)


def gather_kernel(*refs):
    got, (q_out, k_out, v_out) = refs[:4], refs[4:]
    for i in range(4):
        for klass in range(4):
            q_out[klass, i * LOC:(i + 1) * LOC, :] = got[i][klass * LOC:(klass + 1) * LOC, :]
        k_out[i * TOK:(i + 1) * TOK, :] = got[i][TOK:2 * TOK, :]
        v_out[:, i * TOK:(i + 1) * TOK] = got[i][2 * TOK:, :].T


def gather_group(messages):
    full = pl.BlockSpec(memory_space=pltpu.VMEM)
    return pl.pallas_call(
        gather_kernel,
        in_specs=[full] * 4,
        out_specs=[full] * 3,
        out_shape=[
            jax.ShapeDtypeStruct((4, 4 * LOC, HEAD_DIM), jnp.bfloat16),
            jax.ShapeDtypeStruct((4 * TOK, HEAD_DIM), jnp.bfloat16),
            jax.ShapeDtypeStruct((HEAD_DIM, 4 * TOK), jnp.bfloat16),
        ],
        compiler_params=pltpu.CompilerParams(vmem_limit_bytes=16 * 2**20),
        name="gather_group",
    )(*messages)


def attend_kernel(klass_ref, source_ref, *refs):
    queries, keys, values, out_ref = refs[:4], refs[4:8], refs[8:12], refs[12]
    half = pl.program_id(0)
    step = 512
    q = jnp.concatenate([jnp.where(half == 0, queries[i][0], queries[i + 2][0]) for i in range(2)], axis=0)
    scaled = q.astype(jnp.float32) * LOG2_SCALE
    high = scaled.astype(jnp.bfloat16)
    low = (scaled - high.astype(jnp.float32)).astype(jnp.bfloat16)
    rhs = jnp.concatenate([high, low], axis=1)
    top = total = acc = None
    for g in range(4):
        for at in range(0, 4 * TOK, step):
            k = keys[g][at:at + step, :]
            scores = lax.dot_general(jnp.concatenate([k, k], axis=1), rhs, (((1,), (1,)), ((), ())),
                                     preferred_element_type=jnp.float32)
            own = jnp.max(scores, axis=0, keepdims=True)
            new_top = own if top is None else jnp.maximum(top, own)
            weights = jnp.exp2(scores - new_top)
            part = jnp.sum(weights, axis=0, keepdims=True)
            out = jnp.dot(values[g][:, at:at + step], weights.astype(jnp.bfloat16),
                          preferred_element_type=jnp.float32)
            if top is None:
                total, acc = part, out
            else:
                fade = jnp.exp2(top - new_top)
                total, acc = total * fade + part, acc * fade + out
            top = new_top
    done = (acc / total).T.astype(jnp.bfloat16)
    for i in range(8):
        row = pl.multiple_of(source_ref[8 * half + i] * LOC, LOC)
        out_ref[pl.ds(row, LOC), :] = done[i * LOC:(i + 1) * LOC, :]


def attend(klass, source, groups):
    full = pl.BlockSpec(memory_space=pltpu.VMEM)
    rows = SEQ * LOC
    grid_spec = pltpu.PrefetchScalarGridSpec(
        num_scalar_prefetch=2,
        grid=(2,),
        in_specs=[pl.BlockSpec((1, 4 * LOC, HEAD_DIM), lambda i, klass, source: (klass[0], 0, 0))] * 4
        + [pl.BlockSpec((4 * TOK, HEAD_DIM), lambda i, klass, source: (0, 0))] * 4
        + [pl.BlockSpec((HEAD_DIM, 4 * TOK), lambda i, klass, source: (0, 0))] * 4,
        out_specs=pl.BlockSpec((rows, HEAD_DIM), lambda i, klass, source: (0, 0)),
    )
    return pl.pallas_call(
        attend_kernel,
        grid_spec=grid_spec,
        out_shape=jax.ShapeDtypeStruct((rows, HEAD_DIM), jnp.bfloat16),
        cost_estimate=pl.CostEstimate(flops=4 * rows * SEQ * TOK * HEAD_DIM, transcendentals=rows * SEQ * TOK,
                                      bytes_accessed=2 * 3 * SEQ * TOK * HEAD_DIM),
        compiler_params=pltpu.CompilerParams(vmem_limit_bytes=32 * 2**20),
        name="attend",
    )(klass, source, *[g[0] for g in groups], *[g[1] for g in groups], *[g[2] for g in groups])


def merge_kernel(shift_ref, *refs):
    blocks, out_ref = refs[:5], refs[5]
    row = lax.broadcasted_iota(jnp.int32, (HEAD_DIM, OUT_COLS), 0)
    col = lax.broadcasted_iota(jnp.int32, (HEAD_DIM, OUT_COLS), 1)
    picks = [jnp.where(col == row + shift_ref[j], 1.0, 0.0).astype(jnp.bfloat16) for j in range(5)]
    block = jnp.concatenate([ref[...] for ref in blocks], axis=1)
    out_ref[...] = jnp.dot(block, jnp.concatenate(picks, axis=0),
                           preferred_element_type=jnp.float32).astype(jnp.bfloat16)


def merge(shift, blocks):
    rows = SEQ * LOC
    full = pl.BlockSpec(memory_space=pltpu.VMEM)
    return pl.pallas_call(
        merge_kernel,
        in_specs=[pl.BlockSpec(memory_space=pltpu.SMEM)] + [full] * 5,
        out_specs=full,
        out_shape=jax.ShapeDtypeStruct((rows, OUT_COLS), jnp.bfloat16),
        compiler_params=pltpu.CompilerParams(vmem_limit_bytes=24 * 2**20),
        name="merge",
    )(shift, *blocks)


def exchange_and_attend(queries, key_rows, value_rows):
    axes = ("dp", "seq")
    core = lax.axis_index("dp") % 2
    seq = lax.axis_index("seq")
    send = jnp.asarray(SEND)[core, seq]
    source = jnp.asarray(SOURCE)[core, seq]
    shift = jnp.asarray(SHIFT)[core, seq]
    last = jnp.asarray(LAST)[core, seq]

    messages = pack(send, queries, key_rows, value_rows)
    got = [messages[0]]
    for r in range(1, 16):
        perm = pairs(lambda s: turn(s, ROTATIONS[r]), lambda core, s, t: HEAD_OF[core, t] >= 0)
        got.append(lax.ppermute(messages[r], axes, perm))
    groups = [gather_group(got[i:i + 4]) for i in range(0, 16, 4)]

    blocks = []
    for flip in XORS:
        klass = ((seq // 4) ^ flip).reshape(1)
        out = attend(klass, source, groups)
        if flip:
            perm = pairs(lambda s: ((s // 4) ^ flip) * 4 + s % 4, lambda core, s, t: HEAD_OF[core, s] >= 0)
            out = lax.ppermute(out, axes, perm)
        blocks.append(out)
    tail = blocks[0]
    for j in range(1, 4):
        tail = jnp.where(last == j, blocks[j], tail)
    perm = pairs(lambda s: s + 1 if s % 4 < 3 else None, lambda core, s, t: True)
    blocks.append(lax.ppermute(tail, axes, perm))
    return merge(shift, blocks)


def solution(mesh):
    placed = (P(("dp", "seq"), None), P(("dp", "seq"), None), P(("dp", "seq"), None))
    return jax.shard_map(exchange_and_attend, mesh=mesh, in_specs=placed, out_specs=P("dp", "seq"), check_vma=False)
```

```python
import math

import jax
import jax.numpy as jnp
import numpy as np
from jax import lax
from jax.experimental import pallas as pl
from jax.experimental.pallas import tpu as pltpu
from jax.sharding import PartitionSpec as P


HEAD_DIM = 128
HEADS = 13
SEQ = 16
TOK = 256
LOC = 64
OUT_COLS = 416
FAR = 1 << 20
LOG2_SCALE = math.log2(math.e) / math.sqrt(HEAD_DIM)


IDLE = (((), (0,), (1,), (3,)), ((), (3,), (2,), (0,)))
CHUNK_HEADS = ((0, 1, 2, 3), (4, 5, 6), (7, 8, 9), (10, 11, 12))

ROTATIONS = ((0, 0), (1, 0), (0, 1), (0, 7), (1, 1), (1, 7), (0, 2), (0, 6), (1, 2), (1, 6), (0, 3), (0, 5), (1, 3),
             (1, 5), (0, 4), (1, 4))
XORS = (3, 1, 2, 0)


def place_heads():
    head_of = np.full((2, SEQ), -1, np.int32)
    for core in range(2):
        for chunk in range(4):
            places = [p for p in range(4) if p not in IDLE[core][chunk]]
            for place, head in zip(places, CHUNK_HEADS[chunk]):
                head_of[core, place * 4 + chunk] = head
    return head_of


HEAD_OF = place_heads()


def turn(seq, rotation, sign=1):
    dx, dz = rotation
    return ((seq // 8) ^ dx) * 8 + (seq % 8 + sign * dz) % 8


def tables():
    send = np.zeros((2, SEQ, 16), np.int32)
    source = np.zeros((2, SEQ, 16), np.int32)
    shift = np.full((2, SEQ, 5), FAR, np.int32)
    for core in range(2):
        for seq in range(SEQ):
            for r, rotation in enumerate(ROTATIONS):
                send[core, seq, r] = max(HEAD_OF[core, turn(seq, rotation)], 0)
                source[core, seq, r] = turn(seq, rotation, -1)
            chunk, place = seq % 4, seq // 4
            for j, flip in enumerate(XORS):
                head = HEAD_OF[core, (place ^ flip) * 4 + chunk]
                if head >= 0:
                    shift[core, seq, j] = head * HEAD_DIM - chunk * OUT_COLS
            if chunk > 0:
                shift[core, seq, 4] = CHUNK_HEADS[chunk - 1][-1] * HEAD_DIM - chunk * OUT_COLS
    return send, source, shift


SEND, SOURCE, SHIFT = tables()


def last_index():
    table = np.zeros((2, SEQ), np.int32)
    for core in range(2):
        for seq in range(SEQ):
            chunk, place = seq % 4, seq // 4
            for j, flip in enumerate(XORS):
                if HEAD_OF[core, (place ^ flip) * 4 + chunk] == CHUNK_HEADS[chunk][-1]:
                    table[core, seq] = j
    return table


LAST = last_index()


def pairs(step, active):
    out = []
    for dp in range(16):
        for seq in range(SEQ):
            target = step(seq)
            if target is not None and active(dp % 2, seq, target):
                out.append((dp * SEQ + seq, dp * SEQ + target))
    return out


def pack_kernel(send_ref, q_ref, k_ref, v_ref, *refs):
    outs, q_sorted = refs[:16], refs[16]
    row = lax.broadcasted_iota(jnp.int32, (TOK, TOK), 0)
    col = lax.broadcasted_iota(jnp.int32, (TOK, TOK), 1)
    grid_row, grid_col = col // 64, col % 64
    wanted = ((grid_row % 2) * 2 + grid_col % 2) * LOC + (grid_row // 2) * 32 + grid_col // 2
    order = jnp.where(row == wanted, 1.0, 0.0).astype(jnp.bfloat16)
    q_sorted[...] = jnp.dot(order, q_ref[...], preferred_element_type=jnp.float32).astype(jnp.bfloat16)
    for r in range(16):
        at = pl.ds(pl.multiple_of(send_ref[r] * HEAD_DIM, HEAD_DIM), HEAD_DIM)
        outs[r][0:TOK, :] = q_sorted[:, at]
        outs[r][TOK:2 * TOK, :] = k_ref[:, at]
        outs[r][2 * TOK:, :] = v_ref[:, at]


def pack(send, queries, key_rows, value_rows):
    shape = jax.ShapeDtypeStruct((3 * TOK, HEAD_DIM), jnp.bfloat16)
    full = pl.BlockSpec(memory_space=pltpu.VMEM)
    return pl.pallas_call(
        pack_kernel,
        in_specs=[pl.BlockSpec(memory_space=pltpu.SMEM), full, full, full],
        out_specs=[full] * 16,
        out_shape=[shape] * 16,
        scratch_shapes=[pltpu.VMEM((TOK, HEADS * HEAD_DIM), jnp.bfloat16)],
        compiler_params=pltpu.CompilerParams(vmem_limit_bytes=24 * 2**20),
        name="pack",
    )(send, queries, key_rows, value_rows)


def gather_kernel(*refs):
    got, (q_out, k_out, v_out) = refs[:4], refs[4:]
    for i in range(4):
        for klass in range(4):
            q_out[klass, i * LOC:(i + 1) * LOC, :] = got[i][klass * LOC:(klass + 1) * LOC, :]
        k_out[i * TOK:(i + 1) * TOK, :] = got[i][TOK:2 * TOK, :]
        v_out[:, i * TOK:(i + 1) * TOK] = got[i][2 * TOK:, :].T


def gather_group(messages):
    full = pl.BlockSpec(memory_space=pltpu.VMEM)
    return pl.pallas_call(
        gather_kernel,
        in_specs=[full] * 4,
        out_specs=[full] * 3,
        out_shape=[
            jax.ShapeDtypeStruct((4, 4 * LOC, HEAD_DIM), jnp.bfloat16),
            jax.ShapeDtypeStruct((4 * TOK, HEAD_DIM), jnp.bfloat16),
            jax.ShapeDtypeStruct((HEAD_DIM, 4 * TOK), jnp.bfloat16),
        ],
        compiler_params=pltpu.CompilerParams(vmem_limit_bytes=16 * 2**20),
        name="gather_group",
    )(*messages)


def attend_kernel(klass_ref, source_ref, *refs):
    queries, keys, values, out_ref, stores = refs[:4], refs[4:8], refs[8:12], refs[12], refs[13:]
    width, step = 4 * LOC, 512

    def score(block, g, at, rhs, top):
        k = keys[g][at:at + step, :]
        scores = lax.dot_general(jnp.concatenate([k, k], axis=1), rhs, (((1,), (1,)), ((), ())),
                                 preferred_element_type=jnp.float32)
        stores[block % 2][g * 4 * TOK + at:g * 4 * TOK + at + step, :] = scores
        own = jnp.max(scores.reshape(step // 8, 8, width), axis=0)
        return own if top is None else jnp.maximum(top, own)

    def weigh(block, g, at, top, total, acc):
        weights = jnp.exp2(stores[block % 2][g * 4 * TOK + at:g * 4 * TOK + at + step, :] - top)
        part = jnp.sum(weights.reshape(step // 8, 8, width), axis=0)
        out = jnp.dot(values[g][:, at:at + step], weights.astype(jnp.bfloat16), preferred_element_type=jnp.float32)
        return (part, out) if total is None else (total + part, acc + out)

    top = None
    for block in range(5):
        if block < 4:
            scaled = queries[block][0].astype(jnp.float32) * LOG2_SCALE
            high = scaled.astype(jnp.bfloat16)
            low = (scaled - high.astype(jnp.float32)).astype(jnp.bfloat16)
            rhs = jnp.concatenate([high, low], axis=1)
        new_top = total = acc = None
        for g in range(4):
            for at in range(0, 4 * TOK, step):
                if block < 4:
                    new_top = score(block, g, at, rhs, new_top)
                if block > 0:
                    total, acc = weigh(block - 1, g, at, top, total, acc)
        if block > 0:
            done = (acc / jnp.sum(total, axis=0, keepdims=True)).T.astype(jnp.bfloat16)
            for i in range(4):
                row = pl.multiple_of(source_ref[4 * (block - 1) + i] * LOC, LOC)
                out_ref[pl.ds(row, LOC), :] = done[i * LOC:(i + 1) * LOC, :]
        if block < 4:
            top = jnp.max(new_top, axis=0, keepdims=True)


def attend(klass, source, groups):
    rows = SEQ * LOC
    grid_spec = pltpu.PrefetchScalarGridSpec(
        num_scalar_prefetch=2,
        grid=(1,),
        in_specs=[pl.BlockSpec((1, 4 * LOC, HEAD_DIM), lambda i, klass, source: (klass[0], 0, 0))] * 4
        + [pl.BlockSpec((4 * TOK, HEAD_DIM), lambda i, klass, source: (0, 0))] * 4
        + [pl.BlockSpec((HEAD_DIM, 4 * TOK), lambda i, klass, source: (0, 0))] * 4,
        out_specs=pl.BlockSpec((rows, HEAD_DIM), lambda i, klass, source: (0, 0)),
        scratch_shapes=[pltpu.VMEM((SEQ * TOK, 4 * LOC), jnp.float32)] * 2,
    )
    return pl.pallas_call(
        attend_kernel,
        grid_spec=grid_spec,
        out_shape=jax.ShapeDtypeStruct((rows, HEAD_DIM), jnp.bfloat16),
        cost_estimate=pl.CostEstimate(flops=4 * rows * SEQ * TOK * HEAD_DIM, transcendentals=rows * SEQ * TOK,
                                      bytes_accessed=2 * 3 * SEQ * TOK * HEAD_DIM),
        compiler_params=pltpu.CompilerParams(vmem_limit_bytes=24 * 2**20),
        name="attend",
    )(klass, source, *[g[0] for g in groups], *[g[1] for g in groups], *[g[2] for g in groups])


def merge_kernel(shift_ref, *refs):
    blocks, out_ref = refs[:5], refs[5]
    row = lax.broadcasted_iota(jnp.int32, (HEAD_DIM, OUT_COLS), 0)
    col = lax.broadcasted_iota(jnp.int32, (HEAD_DIM, OUT_COLS), 1)
    picks = [jnp.where(col == row + shift_ref[j], 1.0, 0.0).astype(jnp.bfloat16) for j in range(5)]
    block = jnp.concatenate([ref[...] for ref in blocks], axis=1)
    out_ref[...] = jnp.dot(block, jnp.concatenate(picks, axis=0),
                           preferred_element_type=jnp.float32).astype(jnp.bfloat16)


def merge(shift, blocks):
    rows = SEQ * LOC
    full = pl.BlockSpec(memory_space=pltpu.VMEM)
    return pl.pallas_call(
        merge_kernel,
        in_specs=[pl.BlockSpec(memory_space=pltpu.SMEM)] + [full] * 5,
        out_specs=full,
        out_shape=jax.ShapeDtypeStruct((rows, OUT_COLS), jnp.bfloat16),
        compiler_params=pltpu.CompilerParams(vmem_limit_bytes=24 * 2**20),
        name="merge",
    )(shift, *blocks)


def exchange_and_attend(queries, key_rows, value_rows):
    axes = ("dp", "seq")
    core = lax.axis_index("dp") % 2
    seq = lax.axis_index("seq")
    send = jnp.asarray(SEND)[core, seq]
    source = jnp.asarray(SOURCE)[core, seq]
    shift = jnp.asarray(SHIFT)[core, seq]
    last = jnp.asarray(LAST)[core, seq]

    messages = pack(send, queries, key_rows, value_rows)
    got = [messages[0]]
    for r in range(1, 16):
        near = min(ROTATIONS[r][1], 8 - ROTATIONS[r][1]) <= 2
        perm = pairs(lambda s: turn(s, ROTATIONS[r]), lambda core, s, t: near or HEAD_OF[core, t] >= 0)
        got.append(lax.ppermute(messages[r], axes, perm))
    groups = [gather_group(got[i:i + 4]) for i in range(0, 16, 4)]

    blocks = []
    for flip in XORS:
        klass = ((seq // 4) ^ flip).reshape(1)
        out = attend(klass, source, groups)
        if flip:
            perm = pairs(lambda s: ((s // 4) ^ flip) * 4 + s % 4, lambda core, s, t: True)
            out = lax.ppermute(out, axes, perm)
        blocks.append(out)
    tail = blocks[0]
    for j in range(1, 4):
        tail = jnp.where(last == j, blocks[j], tail)
    perm = pairs(lambda s: turn(s, (0, 1)), lambda core, s, t: True)
    blocks.append(lax.ppermute(tail, axes, perm))
    return merge(shift, blocks)


def solution(mesh):
    placed = (P(("dp", "seq"), None), P(("dp", "seq"), None), P(("dp", "seq"), None))
    return jax.shard_map(exchange_and_attend, mesh=mesh, in_specs=placed, out_specs=P("dp", "seq"), check_vma=False)
```

```python
import math

import jax
import jax.numpy as jnp
from jax import lax
from jax.experimental import pallas as pl
from jax.experimental.pallas import tpu as pltpu
from jax.sharding import PartitionSpec as P


HEAD_DIM = 128
HEADS = 13
SEQ = 16
TOK = 256
LOC = 64
GROUP = 4
WIDE = GROUP * LOC
DEEP = GROUP * TOK
STEP = 512
OUT_COLS = 416
FAR = 1 << 20
LOG2_SCALE = math.log2(math.e) / math.sqrt(HEAD_DIM)


IDLE = ((9, 0, 1, 3), (9, 3, 2, 0))

ROTATIONS = ((0, 0), (1, 0), (0, 1), (0, 7), (1, 1), (1, 7), (0, 2), (0, 6), (1, 2), (1, 6), (0, 3), (0, 5), (1, 3),
             (1, 5), (0, 4), (1, 4))
XORS = (3, 1, 2, 0)


def idle(core, seq):
    place, chunk = seq // 4, seq % 4
    return chunk > 0 and place == IDLE[core][chunk]


def turn(seq, rotation):
    dx, dz = rotation
    return ((seq // 8) ^ dx) * 8 + (seq % 8 + dz) % 8


def pairs(step, active):
    out = []
    for dp in range(16):
        for seq in range(SEQ):
            if active(dp % 2, step(seq)):
                out.append((dp * SEQ + seq, dp * SEQ + step(seq)))
    return out


def pick(index, values):
    out = jnp.int32(values[-1])
    for at in range(len(values) - 1):
        out = jnp.where(index == at, jnp.int32(values[at]), out)
    return out


def idle_place(core, chunk):
    return jnp.where(core == 0, pick(chunk, IDLE[0]), pick(chunk, IDLE[1]))


def head_at(core, seq):
    place, chunk = seq // 4, seq % 4
    late = jnp.where(place > idle_place(core, chunk), 1, 0)
    return jnp.minimum(jnp.where(chunk == 0, place, 1 + 3 * chunk + place - late), HEADS - 1)


def vmem():
    return pl.BlockSpec(memory_space=pltpu.VMEM)


def pack_kernel(q_ref, k_ref, v_ref, *refs):
    outs, queries, sems = refs[:16], refs[16], refs[17]
    core, seq = lax.axis_index("dp") % 2, lax.axis_index("seq")
    first = pltpu.make_async_copy(q_ref, queries, sems.at[32])
    first.start()
    copies, columns = [], []
    for r, (dx, dz) in enumerate(ROTATIONS):
        target = ((seq // 8) ^ dx) * 8 + (seq % 8 + dz) % 8
        at = pl.ds(pl.multiple_of(head_at(core, target) * HEAD_DIM, HEAD_DIM), HEAD_DIM)
        columns.append(at)
        for i, ref in enumerate((k_ref, v_ref)):
            copy = pltpu.make_async_copy(ref.at[:, at], outs[r].at[(i + 1) * TOK:(i + 2) * TOK, :], sems.at[2 * r + i])
            copy.start()
            copies.append(copy)
    row = lax.broadcasted_iota(jnp.int32, (TOK, TOK), 0)
    col = lax.broadcasted_iota(jnp.int32, (TOK, TOK), 1)
    grid_row, grid_col = col // 64, col % 64
    wanted = ((grid_row % 2) * 2 + grid_col % 2) * LOC + (grid_row // 2) * 32 + grid_col // 2
    order = jnp.where(row == wanted, 1.0, 0.0).astype(jnp.bfloat16)
    first.wait()
    for r in range(16):
        outs[r][0:TOK, :] = jnp.dot(order, queries[:, columns[r]],
                                    preferred_element_type=jnp.float32).astype(jnp.bfloat16)
    for copy in copies:
        copy.wait()


def pack(queries, key_rows, value_rows):
    shape = jax.ShapeDtypeStruct((3 * TOK, HEAD_DIM), jnp.bfloat16)
    return pl.pallas_call(
        pack_kernel,
        in_specs=[pl.BlockSpec(memory_space=pl.ANY)] * 3,
        out_specs=[vmem()] * 16,
        out_shape=[shape] * 16,
        scratch_shapes=[pltpu.VMEM((TOK, HEADS * HEAD_DIM), jnp.bfloat16), pltpu.SemaphoreType.DMA((33,))],
        compiler_params=pltpu.CompilerParams(vmem_limit_bytes=16 * 2**20),
        name="pack",
    )(queries, key_rows, value_rows)


def gather_kernel(*refs):
    got, (q_out, k_out, v_out) = refs[:GROUP], refs[GROUP:]
    for i in range(GROUP):
        for klass in range(4):
            q_out[klass, i * LOC:(i + 1) * LOC, :] = got[i][klass * LOC:(klass + 1) * LOC, :]
        k_out[i * TOK:(i + 1) * TOK, :] = got[i][TOK:2 * TOK, :]
        v_out[:, i * TOK:(i + 1) * TOK] = got[i][2 * TOK:, :].T


def gather_group(messages):
    return pl.pallas_call(
        gather_kernel,
        in_specs=[vmem()] * GROUP,
        out_specs=[vmem()] * 3,
        out_shape=[
            jax.ShapeDtypeStruct((4, WIDE, HEAD_DIM), jnp.bfloat16),
            jax.ShapeDtypeStruct((DEEP, HEAD_DIM), jnp.bfloat16),
            jax.ShapeDtypeStruct((HEAD_DIM, DEEP), jnp.bfloat16),
        ],
        compiler_params=pltpu.CompilerParams(vmem_limit_bytes=16 * 2**20),
        name="gather_group",
    )(*messages)


def attend_kernel(stages, groups, known, flip, *refs):
    queries, keys, values, refs = refs[:groups], refs[groups:2 * groups], refs[2 * groups:3 * groups], refs[3 * groups:]
    state = ()
    if known:
        state, refs = refs[:3], refs[3:]
    outs, stores = refs[:-2], refs[-2:]
    seq = lax.axis_index("seq")
    klass = pl.program_id(0) if flip is None else (seq // 4) ^ flip

    units = [[(g, keys_of, at) for g, key_groups in stage for keys_of in key_groups for at in range(0, DEEP, STEP)]
             for stage in stages]
    ready = {}
    tops = {}
    sums = {}

    def score(slot, index, unit):
        g, keys_of, at = unit
        if g not in ready:
            scaled = queries[g][klass].astype(jnp.float32) * LOG2_SCALE
            high = scaled.astype(jnp.bfloat16)
            low = (scaled - high.astype(jnp.float32)).astype(jnp.bfloat16)
            ready[g] = jnp.concatenate([high, low], axis=1)
        k = keys[keys_of][at:at + STEP, :]
        scores = lax.dot_general(jnp.concatenate([k, k], axis=1), ready[g], (((1,), (1,)), ((), ())),
                                 preferred_element_type=jnp.float32)
        stores[slot][index * STEP:(index + 1) * STEP, :] = scores
        own = jnp.max(scores.reshape(STEP // 8, 8, WIDE), axis=0)
        tops[g] = jnp.maximum(tops[g], own) if g in tops else own

    def weigh(slot, index, unit):
        g, keys_of, at = unit
        weights = jnp.exp2(stores[slot][index * STEP:(index + 1) * STEP, :] - tops[g])
        part = jnp.sum(weights.reshape(STEP // 8, 8, WIDE), axis=0)
        out = jnp.dot(values[keys_of][:, at:at + STEP], weights.astype(jnp.bfloat16),
                      preferred_element_type=jnp.float32)
        total, acc = sums.get(g, (None, None))
        sums[g] = (part, out) if total is None else (total + part, acc + out)

    for stage in range(len(stages) + 1):
        scoring = units[stage] if stage < len(stages) else []
        weighing = units[stage - 1] if stage > 0 else []
        steps = max(len(scoring), len(weighing))
        for i in range(steps):
            for n in range(i * len(scoring) // steps, (i + 1) * len(scoring) // steps):
                score(stage % 2, n, scoring[n])
            for n in range(i * len(weighing) // steps, (i + 1) * len(weighing) // steps):
                weigh((stage - 1) % 2, n, weighing[n])
        for g in sorted({unit[0] for unit in weighing}):
            total, acc = sums[g]
            if flip is None:
                outs[0][0, :, g * WIDE:(g + 1) * WIDE] = acc
                outs[1][0, :, g * WIDE:(g + 1) * WIDE] = total
                outs[2][0, :, g * WIDE:(g + 1) * WIDE] = jnp.broadcast_to(tops[g], (8, WIDE))
            else:
                done = (acc / jnp.sum(total, axis=0, keepdims=True)).T.astype(jnp.bfloat16)
                for i in range(GROUP):
                    dx, dz = ROTATIONS[GROUP * g + i]
                    source = ((seq // 8) ^ dx) * 8 + (seq % 8 + 8 - dz) % 8
                    outs[0][pl.ds(pl.multiple_of(source * LOC, LOC), LOC), :] = done[i * LOC:(i + 1) * LOC, :]
        for g in sorted({unit[0] for unit in scoring}):
            top = jnp.max(tops[g], axis=0, keepdims=True)
            if g < known:
                at = slice(g * WIDE, (g + 1) * WIDE)
                old = state[2][klass, 0:1, at]
                top = jnp.maximum(top, old)
                fade = jnp.exp2(old - top)
                sums[g] = (state[1][klass, :, at] * fade, state[0][klass, :, at] * fade)
            tops[g] = top


def attend(stages, groups, known, state, flip):
    count = len(groups)
    rows = SEQ * LOC
    scratch = max(sum(len(key_groups) for _, key_groups in stage) for stage in stages) * DEEP
    if flip is None:
        shapes = [(4, HEAD_DIM, count * WIDE), (4, 8, count * WIDE), (4, 8, count * WIDE)]
        out_shape = [jax.ShapeDtypeStruct(shape, jnp.float32) for shape in shapes]
        out_specs = [pl.BlockSpec((1,) + shape[1:], lambda i: (i, 0, 0)) for shape in shapes]
    else:
        out_shape = [jax.ShapeDtypeStruct((rows, HEAD_DIM), jnp.bfloat16)]
        out_specs = [vmem()]
    work = sum(len(key_groups) for stage in stages for _, key_groups in stage) * WIDE * DEEP * (4 if flip is None else 1)
    return pl.pallas_call(
        lambda *refs: attend_kernel(stages, count, known, flip, *refs),
        grid=(4 if flip is None else 1,),
        in_specs=[vmem()] * (3 * count + len(state)),
        out_specs=out_specs,
        out_shape=out_shape,
        scratch_shapes=[pltpu.VMEM((scratch, WIDE), jnp.float32)] * 2,
        cost_estimate=pl.CostEstimate(flops=4 * work * HEAD_DIM, transcendentals=work,
                                      bytes_accessed=6 * count * DEEP * HEAD_DIM),
        compiler_params=pltpu.CompilerParams(vmem_limit_bytes=16 * 2**20),
        name="attend",
    )(*[g[0] for g in groups], *[g[1] for g in groups], *[g[2] for g in groups], *state)


def last_head_kernel(*refs):
    blocks, out_ref = refs[:4], refs[4]
    core, seq = lax.axis_index("dp") % 2, lax.axis_index("seq")
    wanted = jnp.where(idle_place(core, seq % 4) == 3, 2, 3)
    for flip, block in zip(XORS, blocks):
        @pl.when((seq // 4) ^ flip == wanted)
        def _():
            out_ref[...] = block[...]


def last_head(blocks):
    return pl.pallas_call(
        last_head_kernel,
        in_specs=[vmem()] * 4,
        out_specs=vmem(),
        out_shape=jax.ShapeDtypeStruct((SEQ * LOC, HEAD_DIM), jnp.bfloat16),
        compiler_params=pltpu.CompilerParams(vmem_limit_bytes=8 * 2**20),
        name="last_head",
    )(*blocks)


def merge_kernel(*refs):
    blocks, out_ref = refs[:5], refs[5]
    core, seq = lax.axis_index("dp") % 2, lax.axis_index("seq")
    place, chunk = seq // 4, seq % 4
    rows = out_ref.shape[1]
    at = pl.ds(pl.multiple_of(pl.program_id(0) * rows, rows), rows)
    row = lax.broadcasted_iota(jnp.int32, (OUT_COLS, HEAD_DIM), 0)
    col = lax.broadcasted_iota(jnp.int32, (OUT_COLS, HEAD_DIM), 1)
    shifts = []
    for flip in XORS:
        other = place ^ flip
        shift = head_at(core, other * 4 + chunk) * HEAD_DIM - chunk * OUT_COLS
        shifts.append(jnp.where(other == idle_place(core, chunk), FAR, shift))
    shifts.append(jnp.where(chunk == 0, FAR, 3 * chunk * HEAD_DIM - chunk * OUT_COLS))
    picks = [jnp.where(row == col + shift, 1.0, 0.0).astype(jnp.bfloat16) for shift in shifts]
    block = jnp.concatenate([ref[at, :] for ref in blocks], axis=1)
    out_ref[...] = lax.dot_general(jnp.concatenate(picks, axis=1), block, (((1,), (1,)), ((), ())),
                                   preferred_element_type=jnp.float32).astype(jnp.bfloat16)


def merge(blocks):
    rows = SEQ * LOC
    return pl.pallas_call(
        merge_kernel,
        grid=(4,),
        in_specs=[vmem()] * 5,
        out_specs=pl.BlockSpec((OUT_COLS, rows // 4), lambda i: (0, i)),
        out_shape=jax.ShapeDtypeStruct((OUT_COLS, rows), jnp.bfloat16),
        compiler_params=pltpu.CompilerParams(vmem_limit_bytes=24 * 2**20),
        name="merge",
    )(*blocks).T


def exchange_and_attend(queries, key_rows, value_rows):
    axes = ("dp", "seq")
    messages = pack(queries, key_rows, value_rows)
    got = [messages[0]]
    for r in range(1, 16):
        near = min(ROTATIONS[r][1], 8 - ROTATIONS[r][1]) <= 2
        perm = pairs(lambda s: turn(s, ROTATIONS[r]), lambda core, t: near or not idle(core, t))
        got.append(lax.ppermute(messages[r], axes, perm))
    groups = [gather_group(got[i:i + GROUP]) for i in range(0, 16, GROUP)]

    state = attend([[(0, (0, 1))], [(1, (0, 1))]], groups[:2], 0, [], None)
    state = attend([[(2, (0, 1, 2))], [(0, (2,)), (1, (2,))]], groups[:3], 2, state, None)
    last = [[(3, (0, 1, 2, 3))], [(0, (3,)), (1, (3,)), (2, (3,))]]
    blocks = []
    for flip in XORS:
        out = attend(last, groups, 3, state, flip)[0]
        if flip:
            perm = pairs(lambda s: ((s // 4) ^ flip) * 4 + s % 4, lambda core, t: True)
            out = lax.ppermute(out, axes, perm)
        blocks.append(out)
    tail = last_head(blocks)
    blocks.append(lax.ppermute(tail, axes, pairs(lambda s: turn(s, (0, 1)), lambda core, t: True)))
    return merge(blocks)


def solution(mesh):
    placed = (P(("dp", "seq"), None), P(("dp", "seq"), None), P(("dp", "seq"), None))
    return jax.shard_map(exchange_and_attend, mesh=mesh, in_specs=placed, out_specs=P("dp", "seq"), check_vma=False)
```

```python
import itertools
import math

import jax
import jax.numpy as jnp
from jax import lax
from jax.experimental import pallas as pl
from jax.experimental.pallas import tpu as pltpu
from jax.sharding import PartitionSpec as P


HEAD_DIM = 128
HEADS = 13
SEQ = 16
TOK = 256
LOC = 64
GROUP = 4
WIDE = GROUP * LOC
DEEP = GROUP * TOK
STEP = 512
OUT_COLS = 416
SPLIT = 96
FAR = 1 << 20
LOG2_SCALE = math.log2(math.e) / math.sqrt(HEAD_DIM)


IDLE = ((9, 0, 1, 3), (9, 3, 2, 0))

ROTATIONS = ((0, 0), (1, 0), (0, 1), (0, 7), (1, 1), (1, 7), (0, 2), (0, 6), (1, 2), (1, 6), (0, 3), (0, 5), (1, 3),
             (1, 5), (0, 4), (1, 4))
XORS = (3, 1, 2, 0)
NEAR = 2
FILL_SPREAD = False
FILL_RETURN = True


def idle(core, seq):
    place, chunk = seq // 4, seq % 4
    return chunk > 0 and place == IDLE[core][chunk]


def turn(seq, rotation):
    dx, dz = rotation
    return ((seq // 8) ^ dx) * 8 + (seq % 8 + dz) % 8


def hops(source, target):
    along_z = abs(source % 8 - target % 8)
    return 10 * min(along_z, 8 - along_z) + (source // 8 != target // 8)


def pairs(step, active, fill=False):
    out = []
    for dp in range(16):
        rest = []
        for seq in range(SEQ):
            if active(dp % 2, seq, step(seq)):
                out.append((dp * SEQ + seq, dp * SEQ + step(seq)))
            else:
                rest.append(seq)
        if fill and rest:
            targets = min(itertools.permutations([step(seq) for seq in rest]),
                          key=lambda order: sum(map(hops, rest, order)))
            out.extend((dp * SEQ + seq, dp * SEQ + target) for seq, target in zip(rest, targets))
    return out


def pick(index, values):
    out = jnp.int32(values[-1])
    for at in range(len(values) - 1):
        out = jnp.where(index == at, jnp.int32(values[at]), out)
    return out


def idle_place(core, chunk):
    return jnp.where(core == 0, pick(chunk, IDLE[0]), pick(chunk, IDLE[1]))


def head_at(core, seq):
    place, chunk = seq // 4, seq % 4
    late = jnp.where(place > idle_place(core, chunk), 1, 0)
    return jnp.minimum(jnp.where(chunk == 0, place, 1 + 3 * chunk + place - late), HEADS - 1)


def vmem():
    return pl.BlockSpec(memory_space=pltpu.VMEM)


def pack_kernel(q_ref, k_ref, v_ref, *refs):
    outs, queries, sems = refs[:16], refs[16], refs[17]
    core, seq = lax.axis_index("dp") % 2, lax.axis_index("seq")
    first = pltpu.make_async_copy(q_ref, queries, sems.at[32])
    first.start()
    copies, columns = [], []
    for r, (dx, dz) in enumerate(ROTATIONS):
        target = ((seq // 8) ^ dx) * 8 + (seq % 8 + dz) % 8
        at = pl.ds(pl.multiple_of(head_at(core, target) * HEAD_DIM, HEAD_DIM), HEAD_DIM)
        columns.append(at)
        for i, ref in enumerate((k_ref, v_ref)):
            copy = pltpu.make_async_copy(ref.at[:, at], outs[r].at[(i + 1) * TOK:(i + 2) * TOK, :], sems.at[2 * r + i])
            copy.start()
            copies.append(copy)
    row = lax.broadcasted_iota(jnp.int32, (TOK, TOK), 0)
    col = lax.broadcasted_iota(jnp.int32, (TOK, TOK), 1)
    grid_row, grid_col = col // 64, col % 64
    wanted = ((grid_row % 2) * 2 + grid_col % 2) * LOC + (grid_row // 2) * 32 + grid_col // 2
    order = jnp.where(row == wanted, 1.0, 0.0).astype(jnp.bfloat16)
    first.wait()
    for r in range(16):
        outs[r][0:TOK, :] = jnp.dot(order, queries[:, columns[r]],
                                    preferred_element_type=jnp.float32).astype(jnp.bfloat16)
    for copy in copies:
        copy.wait()


def pack(queries, key_rows, value_rows):
    shape = jax.ShapeDtypeStruct((3 * TOK, HEAD_DIM), jnp.bfloat16)
    return pl.pallas_call(
        pack_kernel,
        in_specs=[pl.BlockSpec(memory_space=pltpu.HBM)] * 3,
        out_specs=[vmem()] * 16,
        out_shape=[shape] * 16,
        scratch_shapes=[pltpu.VMEM((TOK, HEADS * HEAD_DIM), jnp.bfloat16), pltpu.SemaphoreType.DMA((33,))],
        compiler_params=pltpu.CompilerParams(vmem_limit_bytes=16 * 2**20),
        name="pack",
    )(queries, key_rows, value_rows)


def gather_kernel(*refs):
    got, (q_out, k_out, v_out) = refs[:GROUP], refs[GROUP:]
    for i in range(GROUP):
        for klass in range(4):
            q_out[klass, i * LOC:(i + 1) * LOC, :] = got[i][klass * LOC:(klass + 1) * LOC, :]
        k_out[i * TOK:(i + 1) * TOK, :] = got[i][TOK:2 * TOK, :]
        v_out[:, i * TOK:(i + 1) * TOK] = got[i][2 * TOK:, :].T


def gather_group(messages):
    return pl.pallas_call(
        gather_kernel,
        in_specs=[vmem()] * GROUP,
        out_specs=[vmem()] * 3,
        out_shape=[
            jax.ShapeDtypeStruct((4, WIDE, HEAD_DIM), jnp.bfloat16),
            jax.ShapeDtypeStruct((DEEP, HEAD_DIM), jnp.bfloat16),
            jax.ShapeDtypeStruct((HEAD_DIM, DEEP), jnp.bfloat16),
        ],
        compiler_params=pltpu.CompilerParams(vmem_limit_bytes=16 * 2**20),
        name="gather_group",
    )(*messages)


def attend_kernel(stages, groups, known, flips, slots, final, *refs):
    queries, keys, values, refs = refs[:groups], refs[groups:2 * groups], refs[2 * groups:3 * groups], refs[3 * groups:]
    state = ()
    if known:
        state, refs = refs[:3], refs[3:]
    outs, stores = refs[:-2], refs[-2:]
    seq = lax.axis_index("seq")
    classes = range(4) if flips is None else [(seq // 4) ^ flip for flip in flips]
    kept = slots or classes
    stages = [(n, stage) for n in range(len(classes)) for stage in stages]

    units = [[((n, g), keys_of, at) for g, key_groups in stage for keys_of in key_groups
              for at in range(0, DEEP, STEP)] for n, stage in stages]
    ready = {}
    tops = {}
    sums = {}

    def score(slot, index, unit):
        block, keys_of, at = unit
        if block not in ready:
            scaled = queries[block[1]][classes[block[0]]].astype(jnp.float32) * LOG2_SCALE
            high = scaled.astype(jnp.bfloat16)
            low = (scaled - high.astype(jnp.float32)).astype(jnp.bfloat16)
            ready[block] = jnp.concatenate([high, low], axis=1)
        k = keys[keys_of][at:at + STEP, :]
        scores = lax.dot_general(jnp.concatenate([k, k], axis=1), ready[block], (((1,), (1,)), ((), ())),
                                 preferred_element_type=jnp.float32)
        stores[slot][index * STEP:(index + 1) * STEP, :] = scores
        own = jnp.max(scores.reshape(STEP // 8, 8, WIDE), axis=0)
        tops[block] = jnp.maximum(tops[block], own) if block in tops else own

    def weigh(slot, index, unit):
        block, keys_of, at = unit
        weights = jnp.exp2(stores[slot][index * STEP:(index + 1) * STEP, :] - tops[block])
        part = jnp.sum(weights.reshape(STEP // 8, 8, WIDE), axis=0)
        out = jnp.dot(values[keys_of][:, at:at + STEP], weights.astype(jnp.bfloat16),
                      preferred_element_type=jnp.float32)
        total, acc = sums.get(block, (None, None))
        sums[block] = (part, out) if total is None else (total + part, acc + out)

    for stage in range(len(stages) + 1):
        scoring = units[stage] if stage < len(stages) else []
        weighing = units[stage - 1] if stage > 0 else []
        steps = max(len(scoring), len(weighing))
        for i in range(steps):
            for n in range(i * len(scoring) // steps, (i + 1) * len(scoring) // steps):
                score(stage % 2, n, scoring[n])
            for n in range(i * len(weighing) // steps, (i + 1) * len(weighing) // steps):
                weigh((stage - 1) % 2, n, weighing[n])
        for n, g in sorted({unit[0] for unit in weighing}):
            total, acc = sums[n, g]
            if not final:
                outs[0][n, :, g * WIDE:(g + 1) * WIDE] = acc
                outs[1][n, :, g * WIDE:(g + 1) * WIDE] = total
                outs[2][n, :, g * WIDE:(g + 1) * WIDE] = jnp.broadcast_to(tops[n, g], (8, WIDE))
            else:
                done = (acc / jnp.sum(total, axis=0, keepdims=True)).T.astype(jnp.bfloat16)
                for i in range(GROUP):
                    dx, dz = ROTATIONS[GROUP * g + i]
                    source = ((seq // 8) ^ dx) * 8 + (seq % 8 + 8 - dz) % 8
                    outs[0][pl.ds(pl.multiple_of(source * LOC, LOC), LOC), :] = done[i * LOC:(i + 1) * LOC, :]
        for n, g in sorted({unit[0] for unit in scoring}):
            top = jnp.max(tops[n, g], axis=0, keepdims=True)
            if g < known:
                at = slice(g * WIDE, (g + 1) * WIDE)
                old = state[2][kept[n], 0:1, at]
                top = jnp.maximum(top, old)
                fade = jnp.exp2(old - top)
                sums[n, g] = (state[1][kept[n], :, at] * fade, state[0][kept[n], :, at] * fade)
            tops[n, g] = top


def attend(stages, groups, known=0, state=(), flips=None, slots=None, final=False):
    count = len(groups)
    scratch = max(sum(len(key_groups) for _, key_groups in stage) for stage in stages) * DEEP
    classes = 4 if flips is None else len(flips)
    if final:
        out_shape = [jax.ShapeDtypeStruct((SEQ * LOC, HEAD_DIM), jnp.bfloat16)]
    else:
        out_shape = [jax.ShapeDtypeStruct((classes, rows, count * WIDE), jnp.float32) for rows in (HEAD_DIM, 8, 8)]
    work = classes * sum(len(key_groups) for stage in stages for _, key_groups in stage) * WIDE * DEEP
    return pl.pallas_call(
        lambda *refs: attend_kernel(stages, count, known, flips, slots, final, *refs),
        in_specs=[vmem()] * (3 * count + len(state)),
        out_specs=[vmem()] * len(out_shape),
        out_shape=out_shape,
        scratch_shapes=[pltpu.VMEM((scratch, WIDE), jnp.float32)] * 2,
        cost_estimate=pl.CostEstimate(flops=4 * work * HEAD_DIM, transcendentals=work,
                                      bytes_accessed=6 * count * DEEP * HEAD_DIM),
        compiler_params=pltpu.CompilerParams(vmem_limit_bytes=16 * 2**20),
        name="attend",
    )(*[g[0] for g in groups], *[g[1] for g in groups], *[g[2] for g in groups], *state)


def last_head_kernel(*refs):
    blocks, out_ref = refs[:4], refs[4]
    core, seq = lax.axis_index("dp") % 2, lax.axis_index("seq")
    wanted = jnp.where(idle_place(core, seq % 4) == 3, 2, 3)
    row = lax.broadcasted_iota(jnp.int32, (SPLIT, HEAD_DIM), 0)
    col = lax.broadcasted_iota(jnp.int32, (SPLIT, HEAD_DIM), 1)
    picks = [jnp.where((col == row + HEAD_DIM - SPLIT) & ((seq // 4) ^ flip == wanted), 1.0, 0.0).astype(jnp.bfloat16)
             for flip in XORS]
    block = jnp.concatenate([ref[...] for ref in blocks], axis=1)
    out_ref[...] = lax.dot_general(jnp.concatenate(picks, axis=1), block, (((1,), (1,)), ((), ())),
                                   preferred_element_type=jnp.float32).astype(jnp.bfloat16)


def last_head(blocks):
    return pl.pallas_call(
        last_head_kernel,
        in_specs=[vmem()] * 4,
        out_specs=vmem(),
        out_shape=jax.ShapeDtypeStruct((SPLIT, SEQ * LOC), jnp.bfloat16),
        compiler_params=pltpu.CompilerParams(vmem_limit_bytes=8 * 2**20),
        name="last_head",
    )(*blocks)


def own_rows(blocks, rows):
    core, seq = lax.axis_index("dp") % 2, lax.axis_index("seq")
    place, chunk = seq // 4, seq % 4
    row = lax.broadcasted_iota(jnp.int32, (rows, HEAD_DIM), 0)
    col = lax.broadcasted_iota(jnp.int32, (rows, HEAD_DIM), 1)
    picks = []
    for flip in XORS:
        other = place ^ flip
        shift = head_at(core, other * 4 + chunk) * HEAD_DIM - chunk * OUT_COLS
        shift = jnp.where(other == idle_place(core, chunk), FAR, shift)
        picks.append(jnp.where(row == col + shift, 1.0, 0.0).astype(jnp.bfloat16))
    block = jnp.concatenate(blocks, axis=1)
    return lax.dot_general(jnp.concatenate(picks, axis=1), block, (((1,), (1,)), ((), ())),
                           preferred_element_type=jnp.float32)


def merge_kernel(*refs):
    blocks, out_ref = refs[:4], refs[4]
    rows = out_ref.shape[1]
    at = pl.ds(pl.multiple_of(pl.program_id(0) * rows, rows), rows)
    out_ref[...] = own_rows([ref[at, :] for ref in blocks], OUT_COLS).astype(jnp.bfloat16)


def merge(blocks):
    rows = SEQ * LOC
    return pl.pallas_call(
        merge_kernel,
        grid=(2,),
        in_specs=[vmem()] * 4,
        out_specs=pl.BlockSpec((OUT_COLS, rows // 2), lambda i: (0, i)),
        out_shape=jax.ShapeDtypeStruct((OUT_COLS, rows), jnp.bfloat16),
        compiler_params=pltpu.CompilerParams(vmem_limit_bytes=16 * 2**20),
        name="merge",
    )(*blocks)


def finish_kernel(*refs):
    blocks, split, out_ref = refs[:4], refs[4], refs[6]
    chunk = lax.axis_index("seq") % 4
    row = lax.broadcasted_iota(jnp.int32, (HEAD_DIM, SPLIT), 0)
    col = lax.broadcasted_iota(jnp.int32, (HEAD_DIM, SPLIT), 1)
    taken = jnp.where((row == col + 32 - 32 * chunk) & (chunk > 0), 1.0, 0.0).astype(jnp.bfloat16)
    out = own_rows([ref[...] for ref in blocks], HEAD_DIM) + jnp.dot(taken, split[...],
                                                                     preferred_element_type=jnp.float32)
    out_ref[...] = out.astype(jnp.bfloat16)


def finish(blocks, split, merged):
    rows = SEQ * LOC
    return pl.pallas_call(
        finish_kernel,
        grid=(1,),
        in_specs=[vmem()] * 5 + [pl.BlockSpec(memory_space=pltpu.HBM)],
        out_specs=pl.BlockSpec((HEAD_DIM, rows), lambda i: (0, 0)),
        out_shape=jax.ShapeDtypeStruct((OUT_COLS, rows), jnp.bfloat16),
        input_output_aliases={5: 0},
        compiler_params=pltpu.CompilerParams(vmem_limit_bytes=16 * 2**20),
        name="finish",
    )(*blocks, split, merged).T


def exchange_and_attend(queries, key_rows, value_rows):
    axes = ("dp", "seq")
    messages = pack(queries, key_rows, value_rows)
    got = [messages[0]]
    for r in range(1, 16):
        near = min(ROTATIONS[r][1], 8 - ROTATIONS[r][1]) <= NEAR
        perm = pairs(lambda s: turn(s, ROTATIONS[r]), lambda core, s, t: near or not idle(core, t), FILL_SPREAD)
        got.append(lax.ppermute(messages[r], axes, perm))
    groups = [gather_group(got[i:i + GROUP]) for i in range(0, 16, GROUP)]

    first = attend([[(0, (0, 1))], [(1, (0, 1))]], groups[:2])
    second = attend([[(2, (0, 1, 2))], [(0, (2,)), (1, (2,))]], groups[:3], 2, first, XORS[:2])
    blocks = []
    for n, flip in enumerate(XORS):
        if n < 2:
            stages = [[(3, (0, 1, 2, 3))], [(0, (3,)), (1, (3,)), (2, (3,))]]
            out = attend(stages, groups, 3, second, (flip,), (n,), True)[0]
        else:
            stages = [[(3, (0, 1, 2, 3))], [(2, (0, 1, 2, 3))], [(0, (2, 3)), (1, (2, 3))]]
            out = attend(stages, groups, 2, first, (flip,), None, True)[0]
        if flip:
            perm = pairs(lambda s: ((s // 4) ^ flip) * 4 + s % 4, lambda core, s, t: not idle(core, s), FILL_RETURN)
            out = lax.ppermute(out, axes, perm)
        blocks.append(out)
    split = lax.ppermute(last_head(blocks), axes, pairs(lambda s: turn(s, (0, 1)), lambda core, s, t: True))
    merged = merge(blocks)
    return finish(blocks, split, merged)


def solution(mesh):
    placed = (P(("dp", "seq"), None), P(("dp", "seq"), None), P(("dp", "seq"), None))
    return jax.shard_map(exchange_and_attend, mesh=mesh, in_specs=placed, out_specs=P("dp", "seq"), check_vma=False)
```

```python
import itertools
import math

import jax
import jax.numpy as jnp
from jax import lax
from jax.experimental import pallas as pl
from jax.experimental.pallas import tpu as pltpu
from jax.sharding import PartitionSpec as P


HEAD_DIM = 128
HEADS = 13
SEQ = 16
TOK = 256
LOC = 64
GROUP = 4
WIDE = GROUP * LOC
DEEP = GROUP * TOK
STEP = 512
OUT_COLS = 416
SPLIT = 96
FAR = 1 << 20
LOG2_SCALE = math.log2(math.e) / math.sqrt(HEAD_DIM)


IDLE = ((9, 0, 1, 3), (9, 3, 2, 0))

ROTATIONS = ((0, 0), (0, 1), (0, 7), (0, 2), (0, 6), (1, 0), (1, 1), (1, 7), (1, 2), (1, 6), (0, 3), (0, 5), (1, 3),
             (1, 5), (0, 4), (1, 4))
NEAR_Z = range(1, 5)
PASSED = range(5, 10)
FAR_AWAY = range(10, 16)
ROWS = 3 * TOK
XORS = (3, 1, 2, 0)
FILL_RETURN = True


def idle(core, seq):
    place, chunk = seq // 4, seq % 4
    return chunk > 0 and place == IDLE[core][chunk]


def turn(seq, rotation):
    dx, dz = rotation
    return ((seq // 8) ^ dx) * 8 + (seq % 8 + dz) % 8


def hops(source, target):
    along_z = abs(source % 8 - target % 8)
    return 10 * min(along_z, 8 - along_z) + (source // 8 != target // 8)


def pairs(step, active, fill=False):
    out = []
    for dp in range(16):
        rest = []
        for seq in range(SEQ):
            if active(dp % 2, seq, step(seq)):
                out.append((dp * SEQ + seq, dp * SEQ + step(seq)))
            else:
                rest.append(seq)
        if fill and rest:
            targets = min(itertools.permutations([step(seq) for seq in rest]),
                          key=lambda order: sum(map(hops, rest, order)))
            out.extend((dp * SEQ + seq, dp * SEQ + target) for seq, target in zip(rest, targets))
    return out


def pick(index, values):
    out = jnp.int32(values[-1])
    for at in range(len(values) - 1):
        out = jnp.where(index == at, jnp.int32(values[at]), out)
    return out


def idle_place(core, chunk):
    return jnp.where(core == 0, pick(chunk, IDLE[0]), pick(chunk, IDLE[1]))


def head_at(core, seq):
    place, chunk = seq // 4, seq % 4
    late = jnp.where(place > idle_place(core, chunk), 1, 0)
    return jnp.minimum(jnp.where(chunk == 0, place, 1 + 3 * chunk + place - late), HEADS - 1)


def vmem():
    return pl.BlockSpec(memory_space=pltpu.VMEM)


def pack_kernel(q_ref, k_ref, v_ref, *refs):
    outs, queries, sems = refs[:12], refs[12], refs[13]
    core, seq = lax.axis_index("dp") % 2, lax.axis_index("seq")
    first = pltpu.make_async_copy(q_ref, queries, sems.at[32])
    first.start()
    copies, places = [], []
    for r, (dx, dz) in enumerate(ROTATIONS):
        target = ((seq // 8) ^ dx) * 8 + (seq % 8 + dz) % 8
        at = pl.ds(pl.multiple_of(head_at(core, target) * HEAD_DIM, HEAD_DIM), HEAD_DIM)
        if r in PASSED[1:]:
            out, top = outs[r - PASSED[0]], ROWS
        else:
            out, top = outs[r if r <= PASSED[0] else r - 4], 0
        places.append((out, top, at))
        for i, ref in enumerate((k_ref, v_ref)):
            copy = pltpu.make_async_copy(ref.at[:, at], out.at[top + (i + 1) * TOK:top + (i + 2) * TOK, :],
                                         sems.at[2 * r + i])
            copy.start()
            copies.append(copy)
    row = lax.broadcasted_iota(jnp.int32, (TOK, TOK), 0)
    col = lax.broadcasted_iota(jnp.int32, (TOK, TOK), 1)
    grid_row, grid_col = col // 64, col % 64
    wanted = ((grid_row % 2) * 2 + grid_col % 2) * LOC + (grid_row // 2) * 32 + grid_col // 2
    order = jnp.where(row == wanted, 1.0, 0.0).astype(jnp.bfloat16)
    first.wait()
    for out, top, at in places:
        out[top:top + TOK, :] = jnp.dot(order, queries[:, at], preferred_element_type=jnp.float32).astype(jnp.bfloat16)
    for copy in copies:
        copy.wait()


def pack(*arrays):
    arrays = [pltpu.with_memory_space_constraint(array, pltpu.HBM) for array in arrays]
    rows = [ROWS] + [2 * ROWS] * 4 + [ROWS] * 7
    return pl.pallas_call(
        pack_kernel,
        in_specs=[pl.BlockSpec(memory_space=pltpu.HBM)] * 3,
        out_specs=[vmem()] * 12,
        out_shape=[jax.ShapeDtypeStruct((n, HEAD_DIM), jnp.bfloat16) for n in rows],
        scratch_shapes=[pltpu.VMEM((TOK, HEADS * HEAD_DIM), jnp.bfloat16), pltpu.SemaphoreType.DMA((33,))],
        compiler_params=pltpu.CompilerParams(vmem_limit_bytes=16 * 2**20),
        name="pack",
    )(*arrays)


def pass_kernel(*refs):
    for i, ref in enumerate(refs[:-1]):
        refs[-1][i * ROWS:(i + 1) * ROWS, :] = ref[-ROWS:, :]


def pass_on(*arrays):
    return pl.pallas_call(
        pass_kernel,
        in_specs=[vmem()] * len(arrays),
        out_specs=vmem(),
        out_shape=jax.ShapeDtypeStruct((len(arrays) * ROWS, HEAD_DIM), jnp.bfloat16),
        compiler_params=pltpu.CompilerParams(vmem_limit_bytes=8 * 2**20),
        name="pass_on",
    )(*arrays)


def gather_kernel(tops, *refs):
    got, (q_out, k_out, v_out) = refs[:GROUP], refs[GROUP:]
    for i, top in enumerate(tops):
        for klass in range(4):
            at = top + klass * LOC
            q_out[klass, i * LOC:(i + 1) * LOC, :] = got[i][at:at + LOC, :]
        k_out[i * TOK:(i + 1) * TOK, :] = got[i][top + TOK:top + 2 * TOK, :]
        v_out[:, i * TOK:(i + 1) * TOK] = got[i][top + 2 * TOK:top + ROWS, :].T


def gather_group(parts):
    tops = [top for _, top in parts]
    return pl.pallas_call(
        lambda *refs: gather_kernel(tops, *refs),
        in_specs=[vmem()] * GROUP,
        out_specs=[vmem()] * 3,
        out_shape=[
            jax.ShapeDtypeStruct((4, WIDE, HEAD_DIM), jnp.bfloat16),
            jax.ShapeDtypeStruct((DEEP, HEAD_DIM), jnp.bfloat16),
            jax.ShapeDtypeStruct((HEAD_DIM, DEEP), jnp.bfloat16),
        ],
        compiler_params=pltpu.CompilerParams(vmem_limit_bytes=16 * 2**20),
        name="gather_group",
    )(*[part for part, _ in parts])


def attend_kernel(stages, groups, known, flips, slots, final, *refs):
    queries, keys, values, refs = refs[:groups], refs[groups:2 * groups], refs[2 * groups:3 * groups], refs[3 * groups:]
    state = ()
    if known:
        state, refs = refs[:3], refs[3:]
    outs, stores = refs[:-2], refs[-2:]
    seq = lax.axis_index("seq")
    classes = range(4) if flips is None else [(seq // 4) ^ flip for flip in flips]
    kept = slots or classes
    stages = [(n, stage) for n in range(len(classes)) for stage in stages]

    units = [[((n, g), keys_of, at) for g, key_groups in stage for keys_of in key_groups
              for at in range(0, DEEP, STEP)] for n, stage in stages]
    ready = {}
    tops = {}
    sums = {}

    def score(slot, index, unit):
        block, keys_of, at = unit
        if block not in ready:
            scaled = queries[block[1]][classes[block[0]]].astype(jnp.float32) * LOG2_SCALE
            high = scaled.astype(jnp.bfloat16)
            low = (scaled - high.astype(jnp.float32)).astype(jnp.bfloat16)
            ready[block] = jnp.concatenate([high, low], axis=1)
        k = keys[keys_of][at:at + STEP, :]
        scores = lax.dot_general(jnp.concatenate([k, k], axis=1), ready[block], (((1,), (1,)), ((), ())),
                                 preferred_element_type=jnp.float32)
        stores[slot][index * STEP:(index + 1) * STEP, :] = scores
        own = jnp.max(scores.reshape(STEP // 8, 8, WIDE), axis=0)
        tops[block] = jnp.maximum(tops[block], own) if block in tops else own

    def weigh(slot, index, unit):
        block, keys_of, at = unit
        weights = jnp.exp2(stores[slot][index * STEP:(index + 1) * STEP, :] - tops[block])
        part = jnp.sum(weights.reshape(STEP // 8, 8, WIDE), axis=0)
        out = jnp.dot(values[keys_of][:, at:at + STEP], weights.astype(jnp.bfloat16),
                      preferred_element_type=jnp.float32)
        total, acc = sums.get(block, (None, None))
        sums[block] = (part, out) if total is None else (total + part, acc + out)

    for stage in range(len(stages) + 1):
        scoring = units[stage] if stage < len(stages) else []
        weighing = units[stage - 1] if stage > 0 else []
        steps = max(len(scoring), len(weighing))
        for i in range(steps):
            for n in range(i * len(scoring) // steps, (i + 1) * len(scoring) // steps):
                score(stage % 2, n, scoring[n])
            for n in range(i * len(weighing) // steps, (i + 1) * len(weighing) // steps):
                weigh((stage - 1) % 2, n, weighing[n])
        for n, g in sorted({unit[0] for unit in weighing}):
            total, acc = sums[n, g]
            if not final:
                outs[0][n, :, g * WIDE:(g + 1) * WIDE] = acc
                outs[1][n, :, g * WIDE:(g + 1) * WIDE] = total
                outs[2][n, :, g * WIDE:(g + 1) * WIDE] = jnp.broadcast_to(tops[n, g], (8, WIDE))
            else:
                done = (acc / jnp.sum(total, axis=0, keepdims=True)).T.astype(jnp.bfloat16)
                for i in range(GROUP):
                    dx, dz = ROTATIONS[GROUP * g + i]
                    source = ((seq // 8) ^ dx) * 8 + (seq % 8 + 8 - dz) % 8
                    outs[0][pl.ds(pl.multiple_of(source * LOC, LOC), LOC), :] = done[i * LOC:(i + 1) * LOC, :]
        for n, g in sorted({unit[0] for unit in scoring}):
            top = jnp.max(tops[n, g], axis=0, keepdims=True)
            if g < known:
                at = slice(g * WIDE, (g + 1) * WIDE)
                old = state[2][kept[n], 0:1, at]
                top = jnp.maximum(top, old)
                fade = jnp.exp2(old - top)
                sums[n, g] = (state[1][kept[n], :, at] * fade, state[0][kept[n], :, at] * fade)
            tops[n, g] = top


def attend(stages, groups, known=0, state=(), flips=None, slots=None, final=False):
    count = len(groups)
    scratch = max(sum(len(key_groups) for _, key_groups in stage) for stage in stages) * DEEP
    classes = 4 if flips is None else len(flips)
    if final:
        out_shape = [jax.ShapeDtypeStruct((SEQ * LOC, HEAD_DIM), jnp.bfloat16)]
    else:
        out_shape = [jax.ShapeDtypeStruct((classes, rows, count * WIDE), jnp.float32) for rows in (HEAD_DIM, 8, 8)]
    work = classes * sum(len(key_groups) for stage in stages for _, key_groups in stage) * WIDE * DEEP
    return pl.pallas_call(
        lambda *refs: attend_kernel(stages, count, known, flips, slots, final, *refs),
        in_specs=[vmem()] * (3 * count + len(state)),
        out_specs=[vmem()] * len(out_shape),
        out_shape=out_shape,
        scratch_shapes=[pltpu.VMEM((scratch, WIDE), jnp.float32)] * 2,
        cost_estimate=pl.CostEstimate(flops=4 * work * HEAD_DIM, transcendentals=work,
                                      bytes_accessed=6 * count * DEEP * HEAD_DIM),
        compiler_params=pltpu.CompilerParams(vmem_limit_bytes=16 * 2**20),
        name="attend",
    )(*[g[0] for g in groups], *[g[1] for g in groups], *[g[2] for g in groups], *state)


def last_head_kernel(*refs):
    blocks, out_ref = refs[:4], refs[4]
    core, seq = lax.axis_index("dp") % 2, lax.axis_index("seq")
    wanted = jnp.where(idle_place(core, seq % 4) == 3, 2, 3)
    row = lax.broadcasted_iota(jnp.int32, (SPLIT, HEAD_DIM), 0)
    col = lax.broadcasted_iota(jnp.int32, (SPLIT, HEAD_DIM), 1)
    picks = [jnp.where((col == row + HEAD_DIM - SPLIT) & ((seq // 4) ^ flip == wanted), 1.0, 0.0).astype(jnp.bfloat16)
             for flip in XORS]
    block = jnp.concatenate([ref[...] for ref in blocks], axis=1)
    out_ref[...] = lax.dot_general(jnp.concatenate(picks, axis=1), block, (((1,), (1,)), ((), ())),
                                   preferred_element_type=jnp.float32).astype(jnp.bfloat16)


def last_head(blocks):
    return pl.pallas_call(
        last_head_kernel,
        in_specs=[vmem()] * 4,
        out_specs=vmem(),
        out_shape=jax.ShapeDtypeStruct((SPLIT, SEQ * LOC), jnp.bfloat16),
        compiler_params=pltpu.CompilerParams(vmem_limit_bytes=8 * 2**20),
        name="last_head",
    )(*blocks)


def own_rows(blocks, rows):
    core, seq = lax.axis_index("dp") % 2, lax.axis_index("seq")
    place, chunk = seq // 4, seq % 4
    row = lax.broadcasted_iota(jnp.int32, (rows, HEAD_DIM), 0)
    col = lax.broadcasted_iota(jnp.int32, (rows, HEAD_DIM), 1)
    picks = []
    for flip in XORS:
        other = place ^ flip
        shift = head_at(core, other * 4 + chunk) * HEAD_DIM - chunk * OUT_COLS
        shift = jnp.where(other == idle_place(core, chunk), FAR, shift)
        picks.append(jnp.where(row == col + shift, 1.0, 0.0).astype(jnp.bfloat16))
    block = jnp.concatenate(blocks, axis=1)
    return lax.dot_general(jnp.concatenate(picks, axis=1), block, (((1,), (1,)), ((), ())),
                           preferred_element_type=jnp.float32)


def merge_kernel(*refs):
    blocks, out_ref = refs[:4], refs[4]
    rows = out_ref.shape[1]
    at = pl.ds(pl.multiple_of(pl.program_id(0) * rows, rows), rows)
    out_ref[...] = own_rows([ref[at, :] for ref in blocks], OUT_COLS).astype(jnp.bfloat16)


def merge(blocks):
    rows = SEQ * LOC
    return pl.pallas_call(
        merge_kernel,
        grid=(2,),
        in_specs=[vmem()] * 4,
        out_specs=pl.BlockSpec((OUT_COLS, rows // 2), lambda i: (0, i)),
        out_shape=jax.ShapeDtypeStruct((OUT_COLS, rows), jnp.bfloat16),
        compiler_params=pltpu.CompilerParams(vmem_limit_bytes=16 * 2**20),
        name="merge",
    )(*blocks)


def finish_kernel(*refs):
    blocks, split, out_ref = refs[:4], refs[4], refs[6]
    chunk = lax.axis_index("seq") % 4
    row = lax.broadcasted_iota(jnp.int32, (HEAD_DIM, SPLIT), 0)
    col = lax.broadcasted_iota(jnp.int32, (HEAD_DIM, SPLIT), 1)
    taken = jnp.where((row == col + 32 - 32 * chunk) & (chunk > 0), 1.0, 0.0).astype(jnp.bfloat16)
    out = own_rows([ref[...] for ref in blocks], HEAD_DIM) + jnp.dot(taken, split[...],
                                                                     preferred_element_type=jnp.float32)
    out_ref[...] = out.astype(jnp.bfloat16)


def finish(blocks, split, merged):
    rows = SEQ * LOC
    return pl.pallas_call(
        finish_kernel,
        grid=(1,),
        in_specs=[vmem()] * 5 + [pl.BlockSpec(memory_space=pltpu.HBM)],
        out_specs=pl.BlockSpec((HEAD_DIM, rows), lambda i: (0, 0)),
        out_shape=jax.ShapeDtypeStruct((OUT_COLS, rows), jnp.bfloat16),
        input_output_aliases={5: 0},
        compiler_params=pltpu.CompilerParams(vmem_limit_bytes=16 * 2**20),
        name="finish",
    )(*blocks, split, merged).T


def exchange_and_attend(queries, key_rows, value_rows):
    axes = ("dp", "seq")
    messages = pack(queries, key_rows, value_rows)
    everyone = lambda core, s, t: True
    parts = {0: (messages[0], 0)}
    near = []
    for r in NEAR_Z:
        near.append(lax.ppermute(messages[r], axes, pairs(lambda s: turn(s, ROTATIONS[r]), everyone)))
        parts[r] = (near[-1], 0)
    for ranks, arrays in ((PASSED[:3], [messages[5]] + near[:2]), (PASSED[3:], near[2:])):
        passed = lax.ppermute(pass_on(*arrays), axes, pairs(lambda s: turn(s, (1, 0)), everyone))
        for i, r in enumerate(ranks):
            parts[r] = (passed, i * ROWS)
    for r in FAR_AWAY:
        perm = pairs(lambda s: turn(s, ROTATIONS[r]), lambda core, s, t: not idle(core, t))
        parts[r] = (lax.ppermute(messages[r - 4], axes, perm), 0)
    groups = [gather_group([parts[i] for i in range(g, g + GROUP)]) for g in range(0, 16, GROUP)]

    first = attend([[(0, (0, 1))], [(1, (0, 1))]], groups[:2])
    second = attend([[(2, (0, 1, 2))], [(0, (2,)), (1, (2,))]], groups[:3], 2, first, XORS[:2])
    blocks = []
    for n, flip in enumerate(XORS):
        if n < 2:
            stages = [[(3, (0, 1, 2, 3))], [(0, (3,)), (1, (3,)), (2, (3,))]]
            out = attend(stages, groups, 3, second, (flip,), (n,), True)[0]
        else:
            stages = [[(3, (0, 1, 2, 3))], [(2, (0, 1, 2, 3))], [(0, (2, 3)), (1, (2, 3))]]
            out = attend(stages, groups, 2, first, (flip,), None, True)[0]
        if flip:
            perm = pairs(lambda s: ((s // 4) ^ flip) * 4 + s % 4, lambda core, s, t: not idle(core, s), FILL_RETURN)
            out = lax.ppermute(out, axes, perm)
        blocks.append(out)
    split = lax.ppermute(last_head(blocks), axes, pairs(lambda s: turn(s, (0, 1)), lambda core, s, t: True))
    merged = merge(blocks)
    return finish(blocks, split, merged)


def solution(mesh):
    placed = (P(("dp", "seq"), None), P(("dp", "seq"), None), P(("dp", "seq"), None))
    return jax.shard_map(exchange_and_attend, mesh=mesh, in_specs=placed, out_specs=P("dp", "seq"), check_vma=False)
```

```python
import itertools
import math

import jax
import jax.numpy as jnp
from jax import lax
from jax.experimental import pallas as pl
from jax.experimental.pallas import tpu as pltpu
from jax.sharding import PartitionSpec as P


HEAD_DIM = 128
HEADS = 13
SEQ = 16
TOK = 256
LOC = 64
GROUP = 4
WIDE = GROUP * LOC
DEEP = GROUP * TOK
STEP = 1024
OUT_COLS = 416
SPLIT = 96
FAR = 1 << 20
LOG2_SCALE = math.log2(math.e) / math.sqrt(HEAD_DIM)


IDLE = ((9, 0, 1, 3), (9, 3, 2, 0))

ROTATIONS = ((0, 0), (0, 1), (0, 7), (0, 2), (0, 6), (1, 0), (1, 1), (1, 7), (1, 2), (1, 6), (0, 3), (0, 5), (1, 3),
             (1, 5), (0, 4), (1, 4))
NEAR_Z = range(1, 5)
PASSED = range(5, 10)
FAR_AWAY = range(10, 16)
ROWS = 3 * TOK
XORS = (3, 1, 2, 0)
FILL_RETURN = False


def idle(core, seq):
    place, chunk = seq // 4, seq % 4
    return chunk > 0 and place == IDLE[core][chunk]


def turn(seq, rotation):
    dx, dz = rotation
    return ((seq // 8) ^ dx) * 8 + (seq % 8 + dz) % 8


def hops(source, target):
    along_z = abs(source % 8 - target % 8)
    return 10 * min(along_z, 8 - along_z) + (source // 8 != target // 8)


def pairs(step, active, fill=False):
    out = []
    for dp in range(16):
        rest = []
        for seq in range(SEQ):
            if active(dp % 2, seq, step(seq)):
                out.append((dp * SEQ + seq, dp * SEQ + step(seq)))
            else:
                rest.append(seq)
        if fill and rest:
            targets = min(itertools.permutations([step(seq) for seq in rest]),
                          key=lambda order: sum(map(hops, rest, order)))
            out.extend((dp * SEQ + seq, dp * SEQ + target) for seq, target in zip(rest, targets))
    return out


def pick(index, values):
    out = jnp.int32(values[-1])
    for at in range(len(values) - 1):
        out = jnp.where(index == at, jnp.int32(values[at]), out)
    return out


def idle_place(core, chunk):
    return jnp.where(core == 0, pick(chunk, IDLE[0]), pick(chunk, IDLE[1]))


def head_at(core, seq):
    place, chunk = seq // 4, seq % 4
    late = jnp.where(place > idle_place(core, chunk), 1, 0)
    return jnp.minimum(jnp.where(chunk == 0, place, 1 + 3 * chunk + place - late), HEADS - 1)


def vmem():
    return pl.BlockSpec(memory_space=pltpu.VMEM)


def pack_kernel(q_ref, k_ref, v_ref, *refs):
    outs, queries, sems = refs[:12], refs[12], refs[13]
    core, seq = lax.axis_index("dp") % 2, lax.axis_index("seq")
    first = pltpu.make_async_copy(q_ref, queries, sems.at[32])
    first.start()
    copies, places = [], []
    for r, (dx, dz) in enumerate(ROTATIONS):
        target = ((seq // 8) ^ dx) * 8 + (seq % 8 + dz) % 8
        at = pl.ds(pl.multiple_of(head_at(core, target) * HEAD_DIM, HEAD_DIM), HEAD_DIM)
        if r in PASSED[1:]:
            out, top = outs[r - PASSED[0]], ROWS
        else:
            out, top = outs[r if r <= PASSED[0] else r - 4], 0
        places.append((out, top, at))
        for i, ref in enumerate((k_ref, v_ref)):
            copy = pltpu.make_async_copy(ref.at[:, at], out.at[top + (i + 1) * TOK:top + (i + 2) * TOK, :],
                                         sems.at[2 * r + i])
            copy.start()
            copies.append(copy)
    row = lax.broadcasted_iota(jnp.int32, (TOK, TOK), 0)
    col = lax.broadcasted_iota(jnp.int32, (TOK, TOK), 1)
    grid_row, grid_col = col // 64, col % 64
    wanted = ((grid_row % 2) * 2 + grid_col % 2) * LOC + (grid_row // 2) * 32 + grid_col // 2
    order = jnp.where(row == wanted, 1.0, 0.0).astype(jnp.bfloat16)
    first.wait()
    for out, top, at in places:
        out[top:top + TOK, :] = jnp.dot(order, queries[:, at], preferred_element_type=jnp.float32).astype(jnp.bfloat16)
    for copy in copies:
        copy.wait()


def pack(*arrays):
    arrays = [pltpu.with_memory_space_constraint(array, pltpu.HBM) for array in arrays]
    rows = [ROWS] + [2 * ROWS] * 4 + [ROWS] * 7
    return pl.pallas_call(
        pack_kernel,
        in_specs=[pl.BlockSpec(memory_space=pltpu.HBM)] * 3,
        out_specs=[vmem()] * 12,
        out_shape=[jax.ShapeDtypeStruct((n, HEAD_DIM), jnp.bfloat16) for n in rows],
        scratch_shapes=[pltpu.VMEM((TOK, HEADS * HEAD_DIM), jnp.bfloat16), pltpu.SemaphoreType.DMA((33,))],
        compiler_params=pltpu.CompilerParams(vmem_limit_bytes=16 * 2**20),
        name="pack",
    )(*arrays)


def pass_kernel(*refs):
    for i, ref in enumerate(refs[:-1]):
        refs[-1][i * ROWS:(i + 1) * ROWS, :] = ref[-ROWS:, :]


def pass_on(*arrays):
    return pl.pallas_call(
        pass_kernel,
        in_specs=[vmem()] * len(arrays),
        out_specs=vmem(),
        out_shape=jax.ShapeDtypeStruct((len(arrays) * ROWS, HEAD_DIM), jnp.bfloat16),
        compiler_params=pltpu.CompilerParams(vmem_limit_bytes=8 * 2**20),
        name="pass_on",
    )(*arrays)


def gather_kernel(tops, *refs):
    got, (q_out, k_out, v_out) = refs[:GROUP], refs[GROUP:]
    for i, top in enumerate(tops):
        for klass in range(4):
            at = top + klass * LOC
            q_out[klass, i * LOC:(i + 1) * LOC, :] = got[i][at:at + LOC, :]
        k_out[i * TOK:(i + 1) * TOK, :] = got[i][top + TOK:top + 2 * TOK, :]
        v_out[:, i * TOK:(i + 1) * TOK] = got[i][top + 2 * TOK:top + ROWS, :].T


def gather_group(parts):
    tops = [top for _, top in parts]
    return pl.pallas_call(
        lambda *refs: gather_kernel(tops, *refs),
        in_specs=[vmem()] * GROUP,
        out_specs=[vmem()] * 3,
        out_shape=[
            jax.ShapeDtypeStruct((4, WIDE, HEAD_DIM), jnp.bfloat16),
            jax.ShapeDtypeStruct((DEEP, HEAD_DIM), jnp.bfloat16),
            jax.ShapeDtypeStruct((HEAD_DIM, DEEP), jnp.bfloat16),
        ],
        compiler_params=pltpu.CompilerParams(vmem_limit_bytes=16 * 2**20),
        name="gather_group",
    )(*[part for part, _ in parts])


def attend_kernel(stages, groups, known, flips, slots, final, *refs):
    queries, keys, values, refs = refs[:groups], refs[groups:2 * groups], refs[2 * groups:3 * groups], refs[3 * groups:]
    state = ()
    if known:
        state, refs = refs[:3], refs[3:]
    outs, stores = refs[:-2], refs[-2:]
    seq = lax.axis_index("seq")
    classes = range(4) if flips is None else [(seq // 4) ^ flip for flip in flips]
    kept = slots or classes
    stages = [(n, stage) for n in range(len(classes)) for stage in stages]

    units = [[((n, g), keys_of, at) for g, key_groups in stage for keys_of in key_groups
              for at in range(0, DEEP, STEP)] for n, stage in stages]
    ready = {}
    tops = {}
    sums = {}

    def score(slot, index, unit):
        block, keys_of, at = unit
        if block not in ready:
            scaled = queries[block[1]][classes[block[0]]].astype(jnp.float32) * LOG2_SCALE
            high = scaled.astype(jnp.bfloat16)
            low = (scaled - high.astype(jnp.float32)).astype(jnp.bfloat16)
            ready[block] = jnp.concatenate([high, low], axis=1)
        k = keys[keys_of][at:at + STEP, :]
        scores = lax.dot_general(jnp.concatenate([k, k], axis=1), ready[block], (((1,), (1,)), ((), ())),
                                 preferred_element_type=jnp.float32)
        stores[slot][index * STEP:(index + 1) * STEP, :] = scores
        own = jnp.max(scores.reshape(STEP // 8, 8, WIDE), axis=0)
        tops[block] = jnp.maximum(tops[block], own) if block in tops else own

    def weigh(slot, index, unit):
        block, keys_of, at = unit
        weights = jnp.exp2(stores[slot][index * STEP:(index + 1) * STEP, :] - tops[block])
        part = jnp.sum(weights.reshape(STEP // 8, 8, WIDE), axis=0)
        out = jnp.dot(values[keys_of][:, at:at + STEP], weights.astype(jnp.bfloat16),
                      preferred_element_type=jnp.float32)
        total, acc = sums.get(block, (None, None))
        sums[block] = (part, out) if total is None else (total + part, acc + out)

    for stage in range(len(stages) + 1):
        scoring = units[stage] if stage < len(stages) else []
        weighing = units[stage - 1] if stage > 0 else []
        steps = max(len(scoring), len(weighing))
        for i in range(steps):
            for n in range(i * len(scoring) // steps, (i + 1) * len(scoring) // steps):
                score(stage % 2, n, scoring[n])
            for n in range(i * len(weighing) // steps, (i + 1) * len(weighing) // steps):
                weigh((stage - 1) % 2, n, weighing[n])
        for n, g in sorted({unit[0] for unit in weighing}):
            total, acc = sums[n, g]
            if not final:
                outs[0][n, :, g * WIDE:(g + 1) * WIDE] = acc
                outs[1][n, :, g * WIDE:(g + 1) * WIDE] = total
                outs[2][n, :, g * WIDE:(g + 1) * WIDE] = jnp.broadcast_to(tops[n, g], (8, WIDE))
            else:
                done = (acc / jnp.sum(total, axis=0, keepdims=True)).T.astype(jnp.bfloat16)
                for i in range(GROUP):
                    dx, dz = ROTATIONS[GROUP * g + i]
                    source = ((seq // 8) ^ dx) * 8 + (seq % 8 + 8 - dz) % 8
                    outs[0][pl.ds(pl.multiple_of(source * LOC, LOC), LOC), :] = done[i * LOC:(i + 1) * LOC, :]
        for n, g in sorted({unit[0] for unit in scoring}):
            top = jnp.max(tops[n, g], axis=0, keepdims=True)
            if g < known:
                at = slice(g * WIDE, (g + 1) * WIDE)
                old = state[2][kept[n], 0:1, at]
                top = jnp.maximum(top, old)
                fade = jnp.exp2(old - top)
                sums[n, g] = (state[1][kept[n], :, at] * fade, state[0][kept[n], :, at] * fade)
            tops[n, g] = top


def attend(stages, groups, known=0, state=(), flips=None, slots=None, final=False):
    count = len(groups)
    scratch = max(sum(len(key_groups) for _, key_groups in stage) for stage in stages) * DEEP
    classes = 4 if flips is None else len(flips)
    if final:
        out_shape = [jax.ShapeDtypeStruct((SEQ * LOC, HEAD_DIM), jnp.bfloat16)]
    else:
        out_shape = [jax.ShapeDtypeStruct((classes, rows, count * WIDE), jnp.float32) for rows in (HEAD_DIM, 8, 8)]
    work = classes * sum(len(key_groups) for stage in stages for _, key_groups in stage) * WIDE * DEEP
    return pl.pallas_call(
        lambda *refs: attend_kernel(stages, count, known, flips, slots, final, *refs),
        in_specs=[vmem()] * (3 * count + len(state)),
        out_specs=[vmem()] * len(out_shape),
        out_shape=out_shape,
        scratch_shapes=[pltpu.VMEM((scratch, WIDE), jnp.float32)] * 2,
        cost_estimate=pl.CostEstimate(flops=4 * work * HEAD_DIM, transcendentals=work,
                                      bytes_accessed=6 * count * DEEP * HEAD_DIM),
        compiler_params=pltpu.CompilerParams(vmem_limit_bytes=16 * 2**20),
        name="attend",
    )(*[g[0] for g in groups], *[g[1] for g in groups], *[g[2] for g in groups], *state)


def last_head_kernel(*refs):
    blocks, out_ref = refs[:4], refs[4]
    core, seq = lax.axis_index("dp") % 2, lax.axis_index("seq")
    wanted = jnp.where(idle_place(core, seq % 4) == 3, 2, 3)
    row = lax.broadcasted_iota(jnp.int32, (SPLIT, HEAD_DIM), 0)
    col = lax.broadcasted_iota(jnp.int32, (SPLIT, HEAD_DIM), 1)
    picks = [jnp.where((col == row + HEAD_DIM - SPLIT) & ((seq // 4) ^ flip == wanted), 1.0, 0.0).astype(jnp.bfloat16)
             for flip in XORS]
    block = jnp.concatenate([ref[...] for ref in blocks], axis=1)
    out_ref[...] = lax.dot_general(jnp.concatenate(picks, axis=1), block, (((1,), (1,)), ((), ())),
                                   preferred_element_type=jnp.float32).astype(jnp.bfloat16)


def last_head(blocks):
    return pl.pallas_call(
        last_head_kernel,
        in_specs=[vmem()] * 4,
        out_specs=vmem(),
        out_shape=jax.ShapeDtypeStruct((SPLIT, SEQ * LOC), jnp.bfloat16),
        compiler_params=pltpu.CompilerParams(vmem_limit_bytes=8 * 2**20),
        name="last_head",
    )(*blocks)


def own_rows(blocks, rows):
    core, seq = lax.axis_index("dp") % 2, lax.axis_index("seq")
    place, chunk = seq // 4, seq % 4
    row = lax.broadcasted_iota(jnp.int32, (rows, HEAD_DIM), 0)
    col = lax.broadcasted_iota(jnp.int32, (rows, HEAD_DIM), 1)
    picks = []
    for flip in XORS:
        other = place ^ flip
        shift = head_at(core, other * 4 + chunk) * HEAD_DIM - chunk * OUT_COLS
        shift = jnp.where(other == idle_place(core, chunk), FAR, shift)
        picks.append(jnp.where(row == col + shift, 1.0, 0.0).astype(jnp.bfloat16))
    block = jnp.concatenate(blocks, axis=1)
    return lax.dot_general(jnp.concatenate(picks, axis=1), block, (((1,), (1,)), ((), ())),
                           preferred_element_type=jnp.float32)


def merge_kernel(*refs):
    blocks, out_ref = refs[:4], refs[4]
    rows = out_ref.shape[1]
    at = pl.ds(pl.multiple_of(pl.program_id(0) * rows, rows), rows)
    out_ref[...] = own_rows([ref[at, :] for ref in blocks], OUT_COLS).astype(jnp.bfloat16)


def merge(blocks):
    rows = SEQ * LOC
    return pl.pallas_call(
        merge_kernel,
        grid=(2,),
        in_specs=[vmem()] * 4,
        out_specs=pl.BlockSpec((OUT_COLS, rows // 2), lambda i: (0, i)),
        out_shape=jax.ShapeDtypeStruct((OUT_COLS, rows), jnp.bfloat16),
        compiler_params=pltpu.CompilerParams(vmem_limit_bytes=16 * 2**20),
        name="merge",
    )(*blocks)


def finish_kernel(*refs):
    blocks, split, out_ref = refs[:4], refs[4], refs[6]
    chunk = lax.axis_index("seq") % 4
    row = lax.broadcasted_iota(jnp.int32, (HEAD_DIM, SPLIT), 0)
    col = lax.broadcasted_iota(jnp.int32, (HEAD_DIM, SPLIT), 1)
    taken = jnp.where((row == col + 32 - 32 * chunk) & (chunk > 0), 1.0, 0.0).astype(jnp.bfloat16)
    out = own_rows([ref[...] for ref in blocks], HEAD_DIM) + jnp.dot(taken, split[...],
                                                                     preferred_element_type=jnp.float32)
    out_ref[...] = out.astype(jnp.bfloat16)


def finish(blocks, split, merged):
    rows = SEQ * LOC
    return pl.pallas_call(
        finish_kernel,
        grid=(1,),
        in_specs=[vmem()] * 5 + [pl.BlockSpec(memory_space=pltpu.HBM)],
        out_specs=pl.BlockSpec((HEAD_DIM, rows), lambda i: (0, 0)),
        out_shape=jax.ShapeDtypeStruct((OUT_COLS, rows), jnp.bfloat16),
        input_output_aliases={5: 0},
        compiler_params=pltpu.CompilerParams(vmem_limit_bytes=16 * 2**20),
        name="finish",
    )(*blocks, split, merged).T


def exchange_and_attend(queries, key_rows, value_rows):
    axes = ("dp", "seq")
    messages = pack(queries, key_rows, value_rows)
    everyone = lambda core, s, t: True
    parts = {0: (messages[0], 0)}
    near = []
    for r in NEAR_Z:
        near.append(lax.ppermute(messages[r], axes, pairs(lambda s: turn(s, ROTATIONS[r]), everyone)))
        parts[r] = (near[-1], 0)
    for ranks, arrays in ((PASSED[:3], [messages[5]] + near[:2]), (PASSED[3:], near[2:])):
        passed = lax.ppermute(pass_on(*arrays), axes, pairs(lambda s: turn(s, (1, 0)), everyone))
        for i, r in enumerate(ranks):
            parts[r] = (passed, i * ROWS)
    for r in FAR_AWAY:
        perm = pairs(lambda s: turn(s, ROTATIONS[r]), lambda core, s, t: not idle(core, t))
        parts[r] = (lax.ppermute(messages[r - 4], axes, perm), 0)
    groups = [gather_group([parts[i] for i in range(g, g + GROUP)]) for g in range(0, 16, GROUP)]

    first = attend([[(0, (0, 1))], [(1, (0, 1))]], groups[:2])
    second = attend([[(2, (0, 1, 2))], [(0, (2,)), (1, (2,))]], groups[:3], 2, first, XORS[:1])
    blocks = []
    for n, flip in enumerate(XORS):
        if n < 1:
            stages = [[(3, (0, 1, 2, 3))], [(0, (3,)), (1, (3,)), (2, (3,))]]
            out = attend(stages, groups, 3, second, (flip,), (n,), True)[0]
        else:
            stages = [[(3, (0, 1, 2, 3))], [(2, (0, 1, 2, 3))], [(0, (2, 3)), (1, (2, 3))]]
            out = attend(stages, groups, 2, first, (flip,), None, True)[0]
        if flip:
            perm = pairs(lambda s: ((s // 4) ^ flip) * 4 + s % 4, lambda core, s, t: not idle(core, s), FILL_RETURN)
            out = lax.ppermute(out, axes, perm)
        blocks.append(out)
    split = lax.ppermute(last_head(blocks), axes, pairs(lambda s: turn(s, (0, 1)), lambda core, s, t: True))
    merged = merge(blocks)
    return finish(blocks, split, merged)


def solution(mesh):
    placed = (P(("dp", "seq"), None), P(("dp", "seq"), None), P(("dp", "seq"), None))
    return jax.shard_map(exchange_and_attend, mesh=mesh, in_specs=placed, out_specs=P("dp", "seq"), check_vma=False)
```

```python
import itertools
import math

import jax
import jax.numpy as jnp
from jax import lax
from jax.experimental import pallas as pl
from jax.experimental.pallas import tpu as pltpu
from jax.sharding import PartitionSpec as P


HEAD_DIM = 128
HEADS = 13
SEQ = 16
TOK = 256
LOC = 64
GROUP = 4
WIDE = GROUP * LOC
DEEP = GROUP * TOK
STEP = 1024
OUT_COLS = 416
SPLIT = 96
FAR = 1 << 20
LOG2_SCALE = math.log2(math.e) / math.sqrt(HEAD_DIM)


IDLE = ((9, 0, 1, 3), (9, 3, 2, 0))

ROTATIONS = ((0, 0), (0, 1), (0, 7), (0, 2), (0, 6), (1, 0), (1, 1), (1, 7), (1, 2), (1, 6), (0, 3), (0, 5), (1, 3),
             (1, 5), (0, 4), (1, 4))
NEAR_Z = range(1, 5)
PASSED = range(5, 10)
FAR_AWAY = range(10, 16)
ROWS = 3 * TOK
XORS = (3, 1, 2, 0)
FILL_RETURN = False


def idle(core, seq):
    place, chunk = seq // 4, seq % 4
    return chunk > 0 and place == IDLE[core][chunk]


def turn(seq, rotation):
    dx, dz = rotation
    return ((seq // 8) ^ dx) * 8 + (seq % 8 + dz) % 8


def hops(source, target):
    along_z = abs(source % 8 - target % 8)
    return 10 * min(along_z, 8 - along_z) + (source // 8 != target // 8)


def pairs(step, active, fill=False):
    out = []
    for dp in range(16):
        rest = []
        for seq in range(SEQ):
            if active(dp % 2, seq, step(seq)):
                out.append((dp * SEQ + seq, dp * SEQ + step(seq)))
            else:
                rest.append(seq)
        if fill and rest:
            targets = min(itertools.permutations([step(seq) for seq in rest]),
                          key=lambda order: sum(map(hops, rest, order)))
            out.extend((dp * SEQ + seq, dp * SEQ + target) for seq, target in zip(rest, targets))
    return out


def pick(index, values):
    out = jnp.int32(values[-1])
    for at in range(len(values) - 1):
        out = jnp.where(index == at, jnp.int32(values[at]), out)
    return out


def idle_place(core, chunk):
    return jnp.where(core == 0, pick(chunk, IDLE[0]), pick(chunk, IDLE[1]))


def head_at(core, seq):
    place, chunk = seq // 4, seq % 4
    late = jnp.where(place > idle_place(core, chunk), 1, 0)
    return jnp.minimum(jnp.where(chunk == 0, place, 1 + 3 * chunk + place - late), HEADS - 1)


def vmem():
    return pl.BlockSpec(memory_space=pltpu.VMEM)


def pack_kernel(q_ref, k_ref, v_ref, *refs):
    outs, queries, sems = refs[:12], refs[12], refs[13]
    core, seq = lax.axis_index("dp") % 2, lax.axis_index("seq")
    first = pltpu.make_async_copy(q_ref, queries, sems.at[32])
    first.start()
    copies, places = [], []
    for r, (dx, dz) in enumerate(ROTATIONS):
        target = ((seq // 8) ^ dx) * 8 + (seq % 8 + dz) % 8
        at = pl.ds(pl.multiple_of(head_at(core, target) * HEAD_DIM, HEAD_DIM), HEAD_DIM)
        if r in PASSED[1:]:
            out, top = outs[r - PASSED[0]], ROWS
        else:
            out, top = outs[r if r <= PASSED[0] else r - 4], 0
        places.append((out, top, at))
        for i, ref in enumerate((k_ref, v_ref)):
            copy = pltpu.make_async_copy(ref.at[:, at], out.at[top + (i + 1) * TOK:top + (i + 2) * TOK, :],
                                         sems.at[2 * r + i])
            copy.start()
            copies.append(copy)
    row = lax.broadcasted_iota(jnp.int32, (TOK, TOK), 0)
    col = lax.broadcasted_iota(jnp.int32, (TOK, TOK), 1)
    grid_row, grid_col = col // 64, col % 64
    wanted = ((grid_row % 2) * 2 + grid_col % 2) * LOC + (grid_row // 2) * 32 + grid_col // 2
    order = jnp.where(row == wanted, 1.0, 0.0).astype(jnp.bfloat16)
    first.wait()
    for out, top, at in places:
        out[top:top + TOK, :] = jnp.dot(order, queries[:, at], preferred_element_type=jnp.float32).astype(jnp.bfloat16)
    for copy in copies:
        copy.wait()


def pack(*arrays):
    arrays = [pltpu.with_memory_space_constraint(array, pltpu.HBM) for array in arrays]
    rows = [ROWS] + [2 * ROWS] * 4 + [ROWS] * 7
    return pl.pallas_call(
        pack_kernel,
        in_specs=[pl.BlockSpec(memory_space=pltpu.HBM)] * 3,
        out_specs=[vmem()] * 12,
        out_shape=[jax.ShapeDtypeStruct((n, HEAD_DIM), jnp.bfloat16) for n in rows],
        scratch_shapes=[pltpu.VMEM((TOK, HEADS * HEAD_DIM), jnp.bfloat16), pltpu.SemaphoreType.DMA((33,))],
        compiler_params=pltpu.CompilerParams(vmem_limit_bytes=16 * 2**20),
        name="pack",
    )(*arrays)


def pass_kernel(*refs):
    for i, ref in enumerate(refs[:-1]):
        refs[-1][i * ROWS:(i + 1) * ROWS, :] = ref[-ROWS:, :]


def pass_on(*arrays):
    return pl.pallas_call(
        pass_kernel,
        in_specs=[vmem()] * len(arrays),
        out_specs=vmem(),
        out_shape=jax.ShapeDtypeStruct((len(arrays) * ROWS, HEAD_DIM), jnp.bfloat16),
        compiler_params=pltpu.CompilerParams(vmem_limit_bytes=8 * 2**20),
        name="pass_on",
    )(*arrays)


def gather_kernel(tops, *refs):
    got, (q_out, k_out, v_out) = refs[:GROUP], refs[GROUP:]
    for i, top in enumerate(tops):
        for klass in range(4):
            at = top + klass * LOC
            q_out[klass, i * LOC:(i + 1) * LOC, :] = got[i][at:at + LOC, :]
        k_out[i * TOK:(i + 1) * TOK, :] = got[i][top + TOK:top + 2 * TOK, :]
        v_out[:, i * TOK:(i + 1) * TOK] = got[i][top + 2 * TOK:top + ROWS, :].T


def gather_group(parts):
    tops = [top for _, top in parts]
    return pl.pallas_call(
        lambda *refs: gather_kernel(tops, *refs),
        in_specs=[vmem()] * GROUP,
        out_specs=[vmem()] * 3,
        out_shape=[
            jax.ShapeDtypeStruct((4, WIDE, HEAD_DIM), jnp.bfloat16),
            jax.ShapeDtypeStruct((DEEP, HEAD_DIM), jnp.bfloat16),
            jax.ShapeDtypeStruct((HEAD_DIM, DEEP), jnp.bfloat16),
        ],
        compiler_params=pltpu.CompilerParams(vmem_limit_bytes=16 * 2**20),
        name="gather_group",
    )(*[part for part, _ in parts])


def attend_kernel(stages, groups, known, flips, slots, final, *refs):
    queries, keys, values, refs = refs[:groups], refs[groups:2 * groups], refs[2 * groups:3 * groups], refs[3 * groups:]
    state = ()
    if known:
        state, refs = refs[:3], refs[3:]
    outs, stores = refs[:-2], refs[-2:]
    seq = lax.axis_index("seq")
    classes = range(4) if flips is None else [(seq // 4) ^ flip for flip in flips]
    kept = slots or classes
    stages = [(n, stage) for n in range(len(classes)) for stage in stages]

    units = [[((n, g), keys_of, at) for g, key_groups in stage for keys_of in key_groups
              for at in range(0, DEEP, STEP)] for n, stage in stages]
    ready = {}
    tops = {}
    sums = {}

    def score(slot, index, unit):
        block, keys_of, at = unit
        if block not in ready:
            scaled = queries[block[1]][classes[block[0]]].astype(jnp.float32) * LOG2_SCALE
            high = scaled.astype(jnp.bfloat16)
            low = (scaled - high.astype(jnp.float32)).astype(jnp.bfloat16)
            ready[block] = jnp.concatenate([high, low], axis=1)
        k = keys[keys_of][at:at + STEP, :]
        scores = lax.dot_general(jnp.concatenate([k, k], axis=1), ready[block], (((1,), (1,)), ((), ())),
                                 preferred_element_type=jnp.float32)
        stores[slot][index * STEP:(index + 1) * STEP, :] = scores
        own = jnp.max(scores.reshape(STEP // 8, 8, WIDE), axis=0)
        tops[block] = jnp.maximum(tops[block], own) if block in tops else own

    def weigh(slot, index, unit):
        block, keys_of, at = unit
        weights = jnp.exp2(stores[slot][index * STEP:(index + 1) * STEP, :] - tops[block])
        part = jnp.sum(weights.reshape(STEP // 8, 8, WIDE), axis=0)
        out = jnp.dot(values[keys_of][:, at:at + STEP], weights.astype(jnp.bfloat16),
                      preferred_element_type=jnp.float32)
        total, acc = sums.get(block, (None, None))
        sums[block] = (part, out) if total is None else (total + part, acc + out)

    for stage in range(len(stages) + 1):
        scoring = units[stage] if stage < len(stages) else []
        weighing = units[stage - 1] if stage > 0 else []
        steps = max(len(scoring), len(weighing))
        for i in range(steps):
            for n in range(i * len(scoring) // steps, (i + 1) * len(scoring) // steps):
                score(stage % 2, n, scoring[n])
            for n in range(i * len(weighing) // steps, (i + 1) * len(weighing) // steps):
                weigh((stage - 1) % 2, n, weighing[n])
        for n, g in sorted({unit[0] for unit in weighing}):
            total, acc = sums[n, g]
            if not final:
                outs[0][n, :, g * WIDE:(g + 1) * WIDE] = acc
                outs[1][n, :, g * WIDE:(g + 1) * WIDE] = total
                outs[2][n, :, g * WIDE:(g + 1) * WIDE] = jnp.broadcast_to(tops[n, g], (8, WIDE))
            else:
                done = (acc / jnp.sum(total, axis=0, keepdims=True)).T.astype(jnp.bfloat16)
                for i in range(GROUP):
                    dx, dz = ROTATIONS[GROUP * g + i]
                    source = ((seq // 8) ^ dx) * 8 + (seq % 8 + 8 - dz) % 8
                    outs[0][pl.ds(pl.multiple_of(source * LOC, LOC), LOC), :] = done[i * LOC:(i + 1) * LOC, :]
        for n, g in sorted({unit[0] for unit in scoring}):
            top = jnp.max(tops[n, g], axis=0, keepdims=True)
            if g < known:
                at = slice(g * WIDE, (g + 1) * WIDE)
                old = state[2][kept[n], 0:1, at]
                top = jnp.maximum(top, old)
                fade = jnp.exp2(old - top)
                sums[n, g] = (state[1][kept[n], :, at] * fade, state[0][kept[n], :, at] * fade)
            tops[n, g] = top


def attend(stages, groups, known=0, state=(), flips=None, slots=None, final=False):
    count = len(groups)
    scratch = max(sum(len(key_groups) for _, key_groups in stage) for stage in stages) * DEEP
    classes = 4 if flips is None else len(flips)
    if final:
        out_shape = [jax.ShapeDtypeStruct((SEQ * LOC, HEAD_DIM), jnp.bfloat16)]
    else:
        out_shape = [jax.ShapeDtypeStruct((classes, rows, count * WIDE), jnp.float32) for rows in (HEAD_DIM, 8, 8)]
    work = classes * sum(len(key_groups) for stage in stages for _, key_groups in stage) * WIDE * DEEP
    return pl.pallas_call(
        lambda *refs: attend_kernel(stages, count, known, flips, slots, final, *refs),
        in_specs=[vmem()] * (3 * count + len(state)),
        out_specs=[vmem()] * len(out_shape),
        out_shape=out_shape,
        scratch_shapes=[pltpu.VMEM((scratch, WIDE), jnp.float32)] * 2,
        cost_estimate=pl.CostEstimate(flops=4 * work * HEAD_DIM, transcendentals=work,
                                      bytes_accessed=6 * count * DEEP * HEAD_DIM),
        compiler_params=pltpu.CompilerParams(vmem_limit_bytes=16 * 2**20),
        name="attend",
    )(*[g[0] for g in groups], *[g[1] for g in groups], *[g[2] for g in groups], *state)


def last_head_kernel(*refs):
    blocks, out_ref = refs[:4], refs[4]
    core, seq = lax.axis_index("dp") % 2, lax.axis_index("seq")
    wanted = jnp.where(idle_place(core, seq % 4) == 3, 2, 3)
    row = lax.broadcasted_iota(jnp.int32, (SPLIT, HEAD_DIM), 0)
    col = lax.broadcasted_iota(jnp.int32, (SPLIT, HEAD_DIM), 1)
    picks = [jnp.where((col == row + HEAD_DIM - SPLIT) & ((seq // 4) ^ flip == wanted), 1.0, 0.0).astype(jnp.bfloat16)
             for flip in XORS]
    block = jnp.concatenate([ref[...] for ref in blocks], axis=1)
    out_ref[...] = lax.dot_general(jnp.concatenate(picks, axis=1), block, (((1,), (1,)), ((), ())),
                                   preferred_element_type=jnp.float32).astype(jnp.bfloat16)


def last_head(blocks):
    return pl.pallas_call(
        last_head_kernel,
        in_specs=[vmem()] * 4,
        out_specs=vmem(),
        out_shape=jax.ShapeDtypeStruct((SPLIT, SEQ * LOC), jnp.bfloat16),
        compiler_params=pltpu.CompilerParams(vmem_limit_bytes=8 * 2**20),
        name="last_head",
    )(*blocks)


def own_rows(blocks, rows):
    core, seq = lax.axis_index("dp") % 2, lax.axis_index("seq")
    place, chunk = seq // 4, seq % 4
    row = lax.broadcasted_iota(jnp.int32, (rows, HEAD_DIM), 0)
    col = lax.broadcasted_iota(jnp.int32, (rows, HEAD_DIM), 1)
    picks = []
    for flip in XORS:
        other = place ^ flip
        shift = head_at(core, other * 4 + chunk) * HEAD_DIM - chunk * OUT_COLS
        shift = jnp.where(other == idle_place(core, chunk), FAR, shift)
        picks.append(jnp.where(row == col + shift, 1.0, 0.0).astype(jnp.bfloat16))
    block = jnp.concatenate(blocks, axis=1)
    return lax.dot_general(jnp.concatenate(picks, axis=1), block, (((1,), (1,)), ((), ())),
                           preferred_element_type=jnp.float32)


def merge_kernel(*refs):
    blocks, out_ref, top_ref = refs[:4], refs[4], refs[5]
    rows = out_ref.shape[1]
    at = pl.ds(pl.multiple_of(pl.program_id(0) * rows, rows), rows)
    out = own_rows([ref[at, :] for ref in blocks], OUT_COLS).astype(jnp.bfloat16)
    out_ref[...] = out
    top_ref[...] = out[:SPLIT]


def merge(blocks):
    rows = SEQ * LOC
    return pl.pallas_call(
        merge_kernel,
        grid=(2,),
        in_specs=[vmem()] * 4,
        out_specs=[pl.BlockSpec((n, rows // 2), lambda i: (0, i)) for n in (OUT_COLS, SPLIT)],
        out_shape=[jax.ShapeDtypeStruct((n, rows), jnp.bfloat16) for n in (OUT_COLS, SPLIT)],
        compiler_params=pltpu.CompilerParams(vmem_limit_bytes=16 * 2**20),
        name="merge",
    )(*blocks)


def finish_kernel(*refs):
    top, split, _, out_ref = refs
    chunk = lax.axis_index("seq") % 4
    row = lax.broadcasted_iota(jnp.int32, (SPLIT, SPLIT), 0)
    col = lax.broadcasted_iota(jnp.int32, (SPLIT, SPLIT), 1)
    taken = jnp.where((row == col + 32 - 32 * chunk) & (chunk > 0), 1.0, 0.0).astype(jnp.bfloat16)
    out = top[...].astype(jnp.float32) + jnp.dot(taken, split[...], preferred_element_type=jnp.float32)
    out_ref[...] = out.astype(jnp.bfloat16)


def finish(top, split, merged):
    rows = SEQ * LOC
    return pl.pallas_call(
        finish_kernel,
        grid=(1,),
        in_specs=[vmem()] * 2 + [pl.BlockSpec(memory_space=pltpu.HBM)],
        out_specs=pl.BlockSpec((SPLIT, rows), lambda i: (0, 0)),
        out_shape=jax.ShapeDtypeStruct((OUT_COLS, rows), jnp.bfloat16),
        input_output_aliases={2: 0},
        compiler_params=pltpu.CompilerParams(vmem_limit_bytes=16 * 2**20),
        name="finish",
    )(top, split, merged).T


def exchange_and_attend(queries, key_rows, value_rows):
    axes = ("dp", "seq")
    messages = pack(queries, key_rows, value_rows)
    everyone = lambda core, s, t: True
    parts = {0: (messages[0], 0)}
    near = []
    for r in NEAR_Z:
        near.append(lax.ppermute(messages[r], axes, pairs(lambda s: turn(s, ROTATIONS[r]), everyone)))
        parts[r] = (near[-1], 0)
    for ranks, arrays in ((PASSED[:3], [messages[5]] + near[:2]), (PASSED[3:], near[2:])):
        passed = lax.ppermute(pass_on(*arrays), axes, pairs(lambda s: turn(s, (1, 0)), everyone))
        for i, r in enumerate(ranks):
            parts[r] = (passed, i * ROWS)
    for r in FAR_AWAY:
        perm = pairs(lambda s: turn(s, ROTATIONS[r]), lambda core, s, t: not idle(core, t))
        parts[r] = (lax.ppermute(messages[r - 4], axes, perm), 0)
    groups = [gather_group([parts[i] for i in range(g, g + GROUP)]) for g in range(0, 16, GROUP)]

    first = attend([[(0, (0, 1))], [(1, (0, 1))]], groups[:2])
    second = attend([[(2, (0, 1, 2))], [(0, (2,)), (1, (2,))]], groups[:3], 2, first, XORS[:1])
    blocks = []
    for n, flip in enumerate(XORS):
        if n < 1:
            stages = [[(3, (0, 1, 2, 3))], [(0, (3,)), (1, (3,)), (2, (3,))]]
            out = attend(stages, groups, 3, second, (flip,), (n,), True)[0]
        else:
            stages = [[(3, (0, 1, 2, 3))], [(2, (0, 1, 2, 3))], [(0, (2, 3)), (1, (2, 3))]]
            out = attend(stages, groups, 2, first, (flip,), None, True)[0]
        if flip:
            perm = pairs(lambda s: ((s // 4) ^ flip) * 4 + s % 4, lambda core, s, t: not idle(core, s), FILL_RETURN)
            out = lax.ppermute(out, axes, perm)
        blocks.append(out)
    split = lax.ppermute(last_head(blocks), axes, pairs(lambda s: turn(s, (0, 1)), lambda core, s, t: True))
    merged, top = merge(blocks)
    return finish(top, split, merged)


def solution(mesh):
    placed = (P(("dp", "seq"), None), P(("dp", "seq"), None), P(("dp", "seq"), None))
    return jax.shard_map(exchange_and_attend, mesh=mesh, in_specs=placed, out_specs=P("dp", "seq"), check_vma=False)
```
